32 devices in a mesh: blk: 16 (over z, y, x), edge: 2 (over core).
Axes of the slice: x: 2, y: 2, z: 4, core: 2. Of those that a mesh axis runs over, the one named last changes fastest.
Arguments:
- node_feat: bfloat16 [512, 128], P(('blk', 'edge')), may hold values from -6 to 6
- coords: bfloat16 [3, 512], P(None, ('blk', 'edge')), may hold values from -4 to 4
- pair_table: int32 [3, 16], replicated, may hold values from 0 to 15, as said below
- w_tgt: bfloat16 [128, 128], replicated, may hold values from -0.375 to 0.375
- w_src: bfloat16 [128, 128], replicated, may hold values from -0.375 to 0.375
- w_dist: float32 [128], replicated, may hold values from -0.8 to 0.8
- edge_bias: float32 [128], replicated, may hold values from -2 to 2
- w_edge: bfloat16 [128, 128], replicated, may hold values from -0.5 to 0.5
- w_gate: float32 [128], replicated, may hold values from -1.5 to 1.5
- w_coord: bfloat16 [128, 128], replicated, may hold values from -0.5 to 0.5
- w_weight: float32 [128], replicated, may hold values from -5 to 5
- w_node_in: bfloat16 [256, 128], replicated, may hold values from -0.375 to 0.375
- w_node_out: bfloat16 [128, 128], replicated, may hold values from -0.5 to 0.5
Outputs:
- new_feat: bfloat16 [512, 128], P(('blk', 'edge'))
- new_coords: float32 [3, 512], P(None, ('blk', 'edge'))
The draws below stay inside these ranges and needn't reach their ends.
Inputs may be any that keep to these rules, and one draw needn't show every extreme that they name: Each row pairs the 16 blocks: pair_table[r, b] = c exactly when pair_table[r, c] = b, and c is never b; no block meets the same partner in two rows.
All inputs are finite; a program needn't handle non-finite values.
Results may differ from the reference program's by a relative error of at most 0.0027.
Values may be sent and summed in bfloat16 or wider, within the bound.
No kernel may reach another device: no remote copies, remote signals or barrier semaphores. Data moves between devices by JAX's collectives and lax.ppermute only.
A program may use at most 128 MiB of HBM per device.

```python
import jax
import jax.numpy as jnp
from jax import lax

F = 128
ROUNDS = 3
BLOCKS = 16
NODES = 512


def draw_pair_table(key, part):
    label_order = jax.random.permutation(jax.random.fold_in(key, 11), BLOCKS).astype(jnp.int32)
    round_labels = jax.random.permutation(jax.random.fold_in(key, 12), BLOCKS - 1)[:ROUNDS].astype(jnp.int32)
    label_of = jnp.zeros((BLOCKS,), jnp.int32).at[label_order].set(jnp.arange(BLOCKS, dtype=jnp.int32))
    last_label = BLOCKS - 1
    own_label = label_of[None, :]
    round_label = round_labels[:, None]
    mirrored = jnp.mod(2 * round_label - own_label, last_label)
    partner_label = jnp.where(own_label == last_label, round_label, jnp.where(own_label == round_label, last_label, mirrored))
    return label_order[partner_label].astype(jnp.int32)


def shard_levels(key, shape, pieces, least, largest):
    gain, own = 1.0, jax.random.fold_in(key, 6)
    for dim, shards_of in pieces:
        draws = jnp.exp(jax.random.uniform(jax.random.fold_in(own, dim), (shards_of,), jnp.float32, least / len(pieces), largest / len(pieces)))
        gain = gain * jnp.repeat(draws, shape[dim] // shards_of).reshape([-1 if axis == dim else 1 for axis in range(len(shape))])
    return gain


def normal_values(rng, extent, width, bound, split=(), kind=jnp.bfloat16):
    array = jax.random.normal(rng, extent, jnp.float32) * width
    if len(split) > 0:
        array = shard_levels(rng, extent, split, -0.22, 0.18) * array
    return jnp.clip(array, min=-bound, max=bound).astype(kind)


def setup_inputs(seed: int = 0) -> dict:
    arg_keys = jax.random.split(jax.random.key(seed), 14)
    node_feat = normal_values(arg_keys[0], (NODES, F), 1.0, 6.0, ((0, 32),))
    coords = normal_values(arg_keys[1], (3, NODES), 1.0, 4.0, ((1, 32),))
    pair_table = draw_pair_table(jax.random.fold_in(arg_keys[13], 71), 0)
    w_tgt = normal_values(arg_keys[3], (F, F), (2 * F) ** -0.5, 0.375)
    w_src = normal_values(arg_keys[4], (F, F), (2 * F) ** -0.5, 0.375)
    w_dist = normal_values(arg_keys[5], (F,), 0.2, 0.8, (), jnp.float32)
    edge_bias = normal_values(arg_keys[6], (F,), 0.5, 2.0, (), jnp.float32)
    w_edge = normal_values(arg_keys[7], (F, F), F ** -0.5, 0.5)
    w_gate = normal_values(arg_keys[8], (F,), 16 ** -0.5, 1.5, (), jnp.float32)
    w_coord = normal_values(arg_keys[9], (F, F), F ** -0.5, 0.5)
    w_weight = normal_values(arg_keys[10], (F,), 1.0, 5.0, (), jnp.float32)
    w_node_in = normal_values(arg_keys[11], (2 * F, F), (2 * F) ** -0.5, 0.375)
    w_node_out = normal_values(arg_keys[12], (F, F), F ** -0.5, 0.5)
    return dict(node_feat=node_feat, coords=coords, pair_table=pair_table, w_tgt=w_tgt, w_src=w_src, w_dist=w_dist, edge_bias=edge_bias, w_edge=w_edge, w_gate=w_gate, w_coord=w_coord, w_weight=w_weight, w_node_in=w_node_in, w_node_out=w_node_out)


def edge_terms(tgt_proj, tgt_place, src_feat, src_place, keep_mask, w_src, w_dist, edge_bias, w_edge, w_gate, w_coord, w_weight):
    src_proj = jnp.dot(src_feat, w_src, preferred_element_type=jnp.float32)
    offset = tgt_place.astype(jnp.float32)[:, :, None] - src_place.astype(jnp.float32)[:, None, :]
    radial = lax.optimization_barrier(jnp.sum(offset * offset, axis=0))
    targets = radial.shape[0]
    sources = radial.shape[1]
    pre_act = tgt_proj[:, None, :] + src_proj[None, :, :] + radial[:, :, None] * w_dist + edge_bias
    hidden = jax.nn.silu(pre_act).astype(jnp.bfloat16).reshape(targets * sources, -1)
    message = jax.nn.silu(jnp.dot(hidden, w_edge, preferred_element_type=jnp.float32))
    edge_gate = jax.nn.sigmoid(lax.optimization_barrier(jnp.sum(message * w_gate, axis=1))).reshape(targets, sources) * keep_mask
    lifted = jax.nn.silu(jnp.dot(message.astype(jnp.bfloat16), w_coord, preferred_element_type=jnp.float32))
    weight = lax.optimization_barrier(jnp.sum(lifted * w_weight, axis=1)).reshape(targets, sources) * keep_mask
    message_sum = lax.optimization_barrier(jnp.sum(message.reshape(targets, sources, -1) * edge_gate[:, :, None], axis=1))
    unit_dir = offset / (jnp.sqrt(radial) + 1.0)
    coord_sum = lax.optimization_barrier(jnp.sum(unit_dir * weight[None], axis=2))
    return (message_sum, coord_sum)

def reference(node_feat, coords, pair_table, w_tgt, w_src, w_dist, edge_bias, w_edge, w_gate, w_coord, w_weight, w_node_in, w_node_out):
    blocks = pair_table.shape[1]
    rounds = pair_table.shape[0]
    feat_width = node_feat.shape[1]
    block_size = node_feat.shape[0] // blocks
    feat_blocks = node_feat.reshape(blocks, block_size, feat_width)
    place_blocks = coords.reshape(3, blocks, block_size).transpose(1, 0, 2)
    mean_scale = 1.0 / ((rounds + 1) * block_size - 1)
    inner_ids = jnp.arange(block_size, dtype=jnp.int32)
    self_keep = (inner_ids[:, None] != inner_ids[None, :]).astype(jnp.float32)
    all_keep = jnp.ones((block_size, block_size), jnp.float32)
    weights = (w_src, w_dist, edge_bias, w_edge, w_gate, w_coord, w_weight)

    def one_block(block_index):
        block_feat = feat_blocks[block_index]
        block_place = place_blocks[block_index]
        tgt_proj = jnp.dot(block_feat, w_tgt, preferred_element_type=jnp.float32)
        message_sum, coord_sum = edge_terms(tgt_proj, block_place, block_feat, block_place, self_keep, *weights)
        for round_step in range(rounds):
            partner = pair_table[round_step, block_index]
            more_msg, more_coord = edge_terms(tgt_proj, block_place, feat_blocks[partner], place_blocks[partner], all_keep, *weights)
            message_sum = message_sum + more_msg
            coord_sum = coord_sum + more_coord
        message_mean = (message_sum * mean_scale).astype(jnp.bfloat16)
        node_pre = jnp.dot(block_feat, w_node_in[:feat_width], preferred_element_type=jnp.float32) + jnp.dot(message_mean, w_node_in[feat_width:], preferred_element_type=jnp.float32)
        node_hidden = jax.nn.silu(node_pre).astype(jnp.bfloat16)
        new_block = (block_feat.astype(jnp.float32) + jnp.dot(node_hidden, w_node_out, preferred_element_type=jnp.float32)).astype(jnp.bfloat16)
        new_place = block_place.astype(jnp.float32) + coord_sum * mean_scale
        return (new_block, new_place)
    new_blocks, new_places = lax.map(one_block, jnp.arange(blocks, dtype=jnp.int32))
    return (new_blocks.reshape(-1, feat_width), new_places.transpose(1, 0, 2).reshape(3, -1))
```

```python
import jax
import jax.numpy as jnp
from jax import lax
from jax.experimental import pallas as pl
from jax.experimental.pallas import tpu as pltpu
from jax.sharding import PartitionSpec as P

F32 = jnp.float32
BF16 = jnp.bfloat16
LANES = 128


def split2(x):
    hi = x.astype(BF16)
    lo = (x - hi.astype(F32)).astype(BF16)
    return hi, lo


def dot(a, b):
    return jnp.dot(a, b, preferred_element_type=F32)


def half_silu(h):
    return h + h * jnp.tanh(h)


def prep_body(
    feat,
    coords,
    w_tgt,
    w_src,
    w_dist,
    edge_bias,
    w_edge,
    w_gate,
    w_coord,
    w_weight,
    w_node,
    a_out,
    w2_out,
    w3_out,
    ww_out,
    place_out,
    node_out,
):
    rows, width = feat.shape
    x = feat[...]
    tgt = (dot(x, w_tgt[...]) + edge_bias[...]) * 0.5
    tgt_hi, tgt_lo = split2(tgt)
    dist = w_dist[...] * 0.5
    d_hi = dist.astype(BF16).astype(F32)
    d_lo = dist - d_hi
    row = lax.broadcasted_iota(jnp.int32, (16, width), 0)
    tail = jnp.where(row == 1, d_lo, jnp.where(row < 3, d_hi, 0.0)).astype(BF16)
    half = jnp.asarray(0.5, BF16)
    stacked = jnp.concatenate([w_src[...] * half, tgt_hi, tgt_lo, tail], axis=0)
    a_out[...] = stacked.T
    w2_out[...] = (w_edge[...] * half).T
    gate = w_gate[...]
    g_hi = gate.astype(BF16).astype(F32)
    g_rows = jnp.where(row == 0, g_hi, jnp.where(row == 1, gate - g_hi, 0.0)).astype(BF16)
    w3_out[...] = jnp.concatenate([(w_coord[...] * half).T, g_rows], axis=0)
    ww_out[...] = jnp.broadcast_to(w_weight[...], (LANES, width)).T
    own = jnp.concatenate([coords[...].astype(F32), jnp.zeros((5, rows), F32)], axis=0)
    own = jnp.concatenate([own, jnp.zeros((8, LANES - rows), F32)], axis=1)
    col = own.T
    for c in range(3):
        place_out[c] = jnp.broadcast_to(col[:rows, c : c + 1], (rows, LANES))
    node_out[...] = dot(x, w_node[:width, :])


def edge_body(
    where,
    table,
    far,
    a_ref,
    w2_ref,
    w3_ref,
    ww_ref,
    place_ref,
    node_ref,
    feat,
    coords,
    w_node,
    w_out,
    feat_out,
    coord_out,
    *,
    edge_parts,
    mean_scale,
):
    rows, width = feat.shape
    rounds = table.shape[0]
    block = where[0]
    part = where[1]
    homes = [block] + [table[r, block] for r in range(rounds)]
    pieces = [far[h * edge_parts + e] for h in homes for e in range(edge_parts)]
    sources = rows * len(pieces)
    parts = sources // LANES
    src = jnp.concatenate([p[:rows] for p in pieces], axis=0)
    src_t = src.T
    spots = jnp.concatenate([p[rows:].astype(F32)[:, :rows] for p in pieces], axis=1)
    lane = lax.broadcasted_iota(jnp.int32, (rows, LANES), 1)
    trow = lax.broadcasted_iota(jnp.int32, (rows, LANES), 0)
    offs, radial, unit, keep, r_hi, r_lo = [], [], [], [], [], []
    for q in range(parts):
        cut = slice(q * LANES, (q + 1) * LANES)
        off = [place_ref[c] - spots[c : c + 1, cut] for c in range(3)]
        rad = off[0] * off[0] + off[1] * off[1] + off[2] * off[2]
        scale = 1.0 / (jnp.sqrt(rad) + 1.0)
        unit.append([o * scale for o in off])
        keep.append(jnp.where(lane + q * LANES == part * rows + trow, 0.0, 1.0))
        hi = rad.astype(BF16).astype(F32)
        r_hi.append(hi)
        r_lo.append(rad - hi)
    a = a_ref[...]
    w2 = w2_ref[...]
    w3 = w3_ref[...]
    urow = lax.broadcasted_iota(jnp.int32, (16, LANES), 0)
    pairs = [(i, q) for i in range(rows) for q in range(parts)]
    group = 2 if len(pairs) % 2 == 0 else 1
    total = jnp.zeros((2 * rows, width), F32)
    weight_rows = {}
    for at in range(0, len(pairs), group):
        members = pairs[at : at + group]
        right = []
        for i, q in members:
            pick = jnp.where(trow == i, 1.0, 0.0).astype(BF16)
            tail = jnp.where(
                urow < 2, r_hi[q][i : i + 1], jnp.where(urow == 2, r_lo[q][i : i + 1], 0.0)
            ).astype(BF16)
            right.append(
                jnp.concatenate(
                    [src_t[:, q * LANES : (q + 1) * LANES], pick, pick, tail], axis=0
                )
            )
        hidden = half_silu(dot(a, jnp.concatenate(right, axis=1))).astype(BF16)
        low = half_silu(dot(w2, hidden)).astype(BF16)
        lifted = dot(w3, low)
        gate = jax.nn.sigmoid(lifted[width : width + 1] + lifted[width + 1 : width + 2])
        lifted = half_silu(lifted[:width])
        left = []
        for m, (i, q) in enumerate(members):
            cut = slice(m * LANES, (m + 1) * LANES)
            weight_rows[i, q] = jnp.sum(lifted[:, cut] * ww_ref[...], axis=0, keepdims=True)
            g = jnp.where(trow == i, gate[:, cut] * keep[q], 0.0)
            left.append(jnp.concatenate(split2(g), axis=0))
        left = jnp.concatenate(left, axis=1)
        total = total + lax.dot_general(
            left, low, (((1,), (1,)), ((), ())), preferred_element_type=F32
        )
    message_mean = ((total[:rows] + total[rows:]) * mean_scale).astype(BF16)
    node_pre = node_ref[...] + dot(message_mean, w_node[width:, :])
    node_hidden = half_silu(node_pre * 0.5).astype(BF16)
    feat_out[...] = (feat[...].astype(F32) + dot(node_hidden, w_out[...])).astype(BF16)
    sums = [jnp.zeros((rows, 1), F32)] * 3
    for q in range(parts):
        weight = jnp.concatenate([weight_rows[i, q] for i in range(rows)], axis=0) * keep[q]
        for c in range(3):
            sums[c] = sums[c] + jnp.sum(unit[q][c] * weight, axis=1, keepdims=True)
    table_cols = jnp.where(lane == 0, sums[0], jnp.where(lane == 1, sums[1], sums[2]))
    coord_out[...] = coords[...].astype(F32) + table_cols.T[:3] * mean_scale


def shards(
    node_feat,
    coords,
    pair_table,
    w_tgt,
    w_src,
    w_dist,
    edge_bias,
    w_edge,
    w_gate,
    w_coord,
    w_weight,
    w_node_in,
    w_node_out,
):
    rows, width = node_feat.shape
    edge_parts = lax.axis_size("edge")
    devices = lax.axis_size("blk") * edge_parts
    rounds = pair_table.shape[0]
    mean_scale = 1.0 / ((rounds + 1) * rows * edge_parts - 1)
    spot = jnp.pad(coords, ((0, 5), (0, width - rows)))
    pack = jnp.concatenate([node_feat, spot], axis=0)
    sent = jnp.broadcast_to(pack[None], (devices,) + pack.shape)
    far = lax.all_to_all(sent, ("blk", "edge"), 0, 0, tiled=True)
    where = jnp.stack([lax.axis_index("blk"), lax.axis_index("edge")]).astype(jnp.int32)
    line = lambda v: v.reshape(1, -1)
    vmem = pl.BlockSpec(memory_space=pltpu.VMEM)
    smem = pl.BlockSpec(memory_space=pltpu.SMEM)
    depth = width + 2 * rows + 16
    prepared = pl.pallas_call(
        prep_body,
        out_shape=(
            jax.ShapeDtypeStruct((width, depth), BF16),
            jax.ShapeDtypeStruct((width, width), BF16),
            jax.ShapeDtypeStruct((width + 16, width), BF16),
            jax.ShapeDtypeStruct((width, LANES), F32),
            jax.ShapeDtypeStruct((3, rows, LANES), F32),
            jax.ShapeDtypeStruct((rows, width), F32),
        ),
        in_specs=[vmem] * 11,
        out_specs=(vmem,) * 6,
        name="prepare",
    )(
        node_feat,
        coords,
        w_tgt,
        w_src,
        line(w_dist),
        line(edge_bias),
        w_edge,
        line(w_gate),
        w_coord,
        line(w_weight),
        w_node_in,
    )

    def body(*refs):
        edge_body(*refs, edge_parts=edge_parts, mean_scale=mean_scale)

    return pl.pallas_call(
        body,
        out_shape=(
            jax.ShapeDtypeStruct((rows, width), BF16),
            jax.ShapeDtypeStruct((3, rows), F32),
        ),
        in_specs=[smem, smem] + [vmem] * 11,
        out_specs=(vmem, vmem),
        name="edges",
    )(where, pair_table, far, *prepared, node_feat, coords, w_node_in, w_node_out)


def solution(mesh):
    whole = P()
    placed = (P(("blk", "edge"), None), P(None, ("blk", "edge"))) + (whole,) * 11
    return jax.shard_map(
        shards,
        mesh=mesh,
        in_specs=placed,
        out_specs=(P(("blk", "edge"), None), P(None, ("blk", "edge"))),
        check_vma=False,
    )
```

```python
import jax
import jax.numpy as jnp
from jax import lax
from jax.experimental import pallas as pl
from jax.experimental.pallas import tpu as pltpu
from jax.sharding import PartitionSpec as P

F32 = jnp.float32
BF16 = jnp.bfloat16
LANES = 128
VMEM_BYTES = 24 * 2**20
WAVE = 8


def split2(x):
    hi = x.astype(BF16)
    lo = (x - hi.astype(F32)).astype(BF16)
    return hi, lo


def dot(a, b):
    return jnp.dot(a, b, preferred_element_type=F32)


def half_silu(h):
    return h + h * jnp.tanh(h)


def pack_body(feat, coords, table, w_dist, edge_bias, w_gate, w_weight, sent, lines, table_out):
    rows, width = feat.shape
    spot = jnp.concatenate([coords[...].astype(F32), jnp.zeros((5, rows), F32)], axis=0)
    spot = jnp.concatenate([spot, jnp.zeros((8, width - rows), F32)], axis=1)
    one = jnp.concatenate([feat[...], spot.astype(BF16)], axis=0)
    sent[...] = jnp.broadcast_to(one[None], sent.shape)
    for k, line in enumerate((w_dist, edge_bias, w_gate, w_weight)):
        lines[k : k + 1, :] = line[...]
    for r in range(table.shape[0]):
        for b in range(table.shape[1]):
            table_out[r, b] = table[r, b]


def edge_body(
    table,
    far,
    lines,
    w_tgt,
    w_src,
    w_edge,
    w_coord,
    w_node,
    w_out,
    feat_out,
    coord_out,
    *,
    edge_parts,
    mean_scale,
):
    rows, width = feat_out.shape
    rounds = table.shape[0]
    block = lax.axis_index("blk")
    part = lax.axis_index("edge")
    blocks = [block] + [table[r, block] for r in range(rounds)]
    pieces = [far[h * edge_parts + e] for h in blocks for e in range(edge_parts)]
    parts = rows * len(pieces) // LANES
    half = jnp.asarray(0.5, BF16)

    src_t = jnp.concatenate([p[:rows] for p in pieces], axis=0).T
    spots = jnp.concatenate([p[rows:].astype(F32)[:, :rows] for p in pieces], axis=1)

    own = far[block * edge_parts + part]
    x = own[:rows]
    w_dist, edge_bias, w_gate, w_weight = (lines[k : k + 1, :] for k in range(4))
    tgt_hi, tgt_lo = split2((dot(x, w_tgt[...]) + edge_bias) * 0.5)
    dist = w_dist * 0.5
    d_hi = dist.astype(BF16).astype(F32)
    urow = lax.broadcasted_iota(jnp.int32, (16, width), 0)
    tail = jnp.where(urow == 1, dist - d_hi, jnp.where(urow < 3, d_hi, 0.0)).astype(BF16)
    a = jnp.concatenate([w_src[...] * half, tgt_hi, tgt_lo, tail], axis=0).T
    w2 = (w_edge[...] * half).T
    gate_w = w_gate
    g_hi = gate_w.astype(BF16).astype(F32)
    g_rows = jnp.where(urow == 0, g_hi, jnp.where(urow == 1, gate_w - g_hi, 0.0)).astype(BF16)
    w3 = jnp.concatenate([(w_coord[...] * half).T, g_rows], axis=0)
    ww = jnp.broadcast_to(w_weight, (LANES, width)).T
    spot = own[rows:].astype(F32)
    col = spot.T[:rows]
    node_part = dot(x, w_node[:width, :])

    lane = lax.broadcasted_iota(jnp.int32, (rows, LANES), 1)
    trow = lax.broadcasted_iota(jnp.int32, (rows, LANES), 0)
    unit, keep, r_hi, r_lo = [], [], [], []
    for q in range(parts):
        cut = slice(q * LANES, (q + 1) * LANES)
        off = [col[:, c : c + 1] - spots[c : c + 1, cut] for c in range(3)]
        rad = off[0] * off[0] + off[1] * off[1] + off[2] * off[2]
        scale = 1.0 / (jnp.sqrt(rad) + 1.0)
        unit.append([o * scale for o in off])
        keep.append(jnp.where(lane + q * LANES == part * rows + trow, 0.0, 1.0))
        hi = rad.astype(BF16).astype(F32)
        r_hi.append(hi)
        r_lo.append(rad - hi)
    lrow = lax.broadcasted_iota(jnp.int32, (16, LANES), 0)
    pairs = [(i, q) for i in range(rows) for q in range(parts)]
    group = 2 if len(pairs) % 2 == 0 else 1
    chunks = [pairs[at : at + group] for at in range(0, len(pairs), group)]
    rights = []
    for members in chunks:
        right = []
        for i, q in members:
            pick = jnp.where(trow == i, 1.0, 0.0).astype(BF16)
            near = jnp.where(
                lrow < 2, r_hi[q][i : i + 1], jnp.where(lrow == 2, r_lo[q][i : i + 1], 0.0)
            ).astype(BF16)
            here = src_t[:, q * LANES : (q + 1) * LANES]
            right.append(jnp.concatenate([here, pick, pick, near], axis=0))
        rights.append(jnp.concatenate(right, axis=1))
    wave = WAVE
    total = jnp.zeros((2 * rows, width), F32)
    weight_rows = {}
    for at in range(0, len(chunks), wave):
        now = range(at, min(at + wave, len(chunks)))
        hidden = [dot(a, rights[k]) for k in now]
        hidden = [half_silu(h).astype(BF16) for h in hidden]
        low = [dot(w2, h) for h in hidden]
        low = [half_silu(h).astype(BF16) for h in low]
        lifted = [dot(w3, h) for h in low]
        gates = [jax.nn.sigmoid(v[width : width + 1] + v[width + 1 : width + 2]) for v in lifted]
        for k, g, m in zip(now, gates, low):
            left = []
            for n, (i, q) in enumerate(chunks[k]):
                cut = slice(n * LANES, (n + 1) * LANES)
                kept = jnp.where(trow == i, g[:, cut] * keep[q], 0.0)
                left.append(jnp.concatenate(split2(kept), axis=0))
            total = total + lax.dot_general(
                jnp.concatenate(left, axis=1),
                m,
                (((1,), (1,)), ((), ())),
                preferred_element_type=F32,
            )
        for k, v in zip(now, lifted):
            v = half_silu(v[:width])
            for n, (i, q) in enumerate(chunks[k]):
                cut = slice(n * LANES, (n + 1) * LANES)
                weight_rows[i, q] = jnp.sum(v[:, cut] * ww, axis=0, keepdims=True)
    message_mean = ((total[:rows] + total[rows:]) * mean_scale).astype(BF16)
    node_pre = node_part + dot(message_mean, w_node[width:, :])
    node_hidden = half_silu(node_pre * 0.5).astype(BF16)
    feat_out[...] = (x.astype(F32) + dot(node_hidden, w_out[...])).astype(BF16)
    sums = [jnp.zeros((rows, 1), F32)] * 3
    for q in range(parts):
        weight = jnp.concatenate([weight_rows[i, q] for i in range(rows)], axis=0) * keep[q]
        for c in range(3):
            sums[c] = sums[c] + jnp.sum(unit[q][c] * weight, axis=1, keepdims=True)
    side = jnp.where(lane == 0, sums[0], jnp.where(lane == 1, sums[1], sums[2]))
    coord_out[...] = spot[:3, :rows] + side.T[:3] * mean_scale


def shards(
    node_feat,
    coords,
    pair_table,
    w_tgt,
    w_src,
    w_dist,
    edge_bias,
    w_edge,
    w_gate,
    w_coord,
    w_weight,
    w_node_in,
    w_node_out,
):
    rows, width = node_feat.shape
    edge_parts = lax.axis_size("edge")
    devices = lax.axis_size("blk") * edge_parts
    rounds = pair_table.shape[0]
    mean_scale = 1.0 / ((rounds + 1) * rows * edge_parts - 1)
    vmem = pl.BlockSpec(memory_space=pltpu.VMEM)
    smem = pl.BlockSpec(memory_space=pltpu.SMEM)
    params = pltpu.CompilerParams(vmem_limit_bytes=VMEM_BYTES)
    line = lambda v: v.reshape(1, -1)
    small = (line(w_dist), line(edge_bias), line(w_gate), line(w_weight))
    hold = lambda v: pltpu.with_memory_space_constraint(v, pltpu.HBM)
    sent, lines, table = pl.pallas_call(
        pack_body,
        out_shape=(
            pltpu.VMEM((devices, rows + 8, width), BF16),
            pltpu.VMEM((8, width), F32),
            pltpu.SMEM(pair_table.shape, pair_table.dtype),
        ),
        in_specs=[vmem] * 2 + [smem] + [vmem] * 4,
        out_specs=(vmem, vmem, smem),
        compiler_params=params,
        name="pack",
    )(*(hold(v) for v in (node_feat, coords, pair_table) + small))
    far = lax.all_to_all(sent, ("blk", "edge"), 0, 0, tiled=True)

    def body(*refs):
        edge_body(*refs, edge_parts=edge_parts, mean_scale=mean_scale)

    return pl.pallas_call(
        body,
        out_shape=(
            jax.ShapeDtypeStruct((rows, width), BF16),
            jax.ShapeDtypeStruct((3, rows), F32),
        ),
        in_specs=[smem] + [vmem] * 8,
        out_specs=(vmem, vmem),
        compiler_params=params,
        name="edges",
    )(
        table,
        far,
        lines,
        w_tgt,
        w_src,
        w_edge,
        w_coord,
        w_node_in,
        w_node_out,
    )


def solution(mesh):
    whole = P()
    placed = (P(("blk", "edge"), None), P(None, ("blk", "edge"))) + (whole,) * 11
    return jax.shard_map(
        shards,
        mesh=mesh,
        in_specs=placed,
        out_specs=(P(("blk", "edge"), None), P(None, ("blk", "edge"))),
        check_vma=False,
    )
```

```python
import jax
import jax.numpy as jnp
from jax import lax
from jax.experimental import pallas as pl
from jax.experimental.pallas import tpu as pltpu
from jax.sharding import PartitionSpec as P

F32 = jnp.float32
BF16 = jnp.bfloat16
LANES = 128
VMEM_BYTES = 24 * 2**20
SPLIT = 2
SLAB = 4


def split2(x):
    hi = x.astype(BF16)
    lo = (x - hi.astype(F32)).astype(BF16)
    return hi, lo


def dot(a, b):
    return jnp.dot(a, b, preferred_element_type=F32)


def half_silu(h):
    return h + h * jnp.tanh(h)


def pack_body(feat, coords, table, w_dist, edge_bias, w_gate, w_weight, sent, lines, table_out):
    rows, width = feat.shape
    spot = jnp.concatenate([coords[...].astype(F32), jnp.zeros((SLAB - 3, rows), F32)], axis=0)
    spot = jnp.concatenate([spot, jnp.zeros((SLAB, width - rows), F32)], axis=1)
    slabs = [feat[k : k + SLAB, :] for k in range(0, rows, SLAB)] + [spot.astype(BF16)]
    for k, slab in enumerate(slabs):
        sent[:, k] = jnp.broadcast_to(slab[None], (sent.shape[0],) + slab.shape)
    for k, line in enumerate((w_dist, edge_bias, w_gate, w_weight)):
        lines[k : k + 1, :] = line[...]
    for r in range(table.shape[0]):
        for b in range(table.shape[1]):
            table_out[r, b] = table[r, b]


def edge_body(
    table,
    far,
    lines,
    w_tgt,
    w_src,
    w_edge,
    w_coord,
    w_node,
    w_out,
    feat_out,
    coord_out,
    *,
    edge_parts,
    mean_scale,
):
    rows, width = feat_out.shape
    rounds = table.shape[0]
    block = lax.axis_index("blk")
    part = lax.axis_index("edge")
    blocks = [block] + [table[r, block] for r in range(rounds)]
    places = [h * edge_parts + e for h in blocks for e in range(edge_parts)]
    slabs = rows // SLAB

    def feats(p):
        return [far[p, k] for k in range(slabs)]

    def spots_of(p):
        return far[p, slabs].astype(F32)

    parts = rows * len(places) // LANES
    half = jnp.asarray(0.5, BF16)

    src_t = jnp.concatenate([f for p in places for f in feats(p)], axis=0).T
    spots = jnp.concatenate([spots_of(p)[:, :rows] for p in places], axis=1)

    own = block * edge_parts + part
    x = jnp.concatenate(feats(own), axis=0)
    w_dist, edge_bias, w_gate, w_weight = (lines[k : k + 1, :] for k in range(4))
    tgt_hi, tgt_lo = split2((dot(x, w_tgt[...]) + edge_bias) * 0.5)
    dist = w_dist * 0.5
    d_hi = dist.astype(BF16).astype(F32)
    urow = lax.broadcasted_iota(jnp.int32, (16, width), 0)
    tail = jnp.where(urow == 1, dist - d_hi, jnp.where(urow < 3, d_hi, 0.0)).astype(BF16)
    a = jnp.concatenate([tgt_hi, tgt_lo, tail], axis=0).T
    src_proj = dot((w_src[...] * half).T, src_t)
    w2 = (w_edge[...] * half).T
    gate_w = w_gate
    g_hi = gate_w.astype(BF16).astype(F32)
    g_rows = jnp.where(urow == 0, g_hi, jnp.where(urow == 1, gate_w - g_hi, 0.0)).astype(BF16)
    w3 = jnp.concatenate([(w_coord[...] * half).T, g_rows], axis=0)
    ww = jnp.broadcast_to(w_weight, (LANES, width)).T
    spot = jnp.concatenate([spots_of(own), jnp.zeros((8 - SLAB, width), F32)], axis=0)
    col = spot.T[:rows]
    node_part = dot(x, w_node[:width, :])

    lane = lax.broadcasted_iota(jnp.int32, (rows, LANES), 1)
    trow = lax.broadcasted_iota(jnp.int32, (rows, LANES), 0)
    unit, keep, r_hi, r_lo = [], [], [], []
    for q in range(parts):
        cut = slice(q * LANES, (q + 1) * LANES)
        off = [col[:, c : c + 1] - spots[c : c + 1, cut] for c in range(3)]
        rad = off[0] * off[0] + off[1] * off[1] + off[2] * off[2]
        scale = 1.0 / (jnp.sqrt(rad) + 1.0)
        unit.append([o * scale for o in off])
        keep.append(jnp.where(lane + q * LANES == part * rows + trow, 0.0, 1.0))
        hi = rad.astype(BF16).astype(F32)
        r_hi.append(hi)
        r_lo.append(rad - hi)
    lrow = lax.broadcasted_iota(jnp.int32, (16, LANES), 0)
    pairs = [(i, q) for i in range(rows) for q in range(parts)]
    group = 2 if len(pairs) % 2 == 0 else 1
    chunks = [pairs[at : at + group] for at in range(0, len(pairs), group)]
    rights = []
    for members in chunks:
        right = []
        for i, q in members:
            pick = jnp.where(trow == i, 1.0, 0.0).astype(BF16)
            near = jnp.where(
                lrow < 2, r_hi[q][i : i + 1], jnp.where(lrow == 2, r_lo[q][i : i + 1], 0.0)
            ).astype(BF16)
            right.append(jnp.concatenate([pick, pick, near], axis=0))
        rights.append(jnp.concatenate(right, axis=1))
    hidden = []
    for members, right in zip(chunks, rights):
        base = [src_proj[:, q * LANES : (q + 1) * LANES] for _, q in members]
        hidden.append(dot(a, right) + jnp.concatenate(base, axis=1))
    hidden = [half_silu(h).astype(BF16) for h in hidden]
    low = [dot(w2, h) for h in hidden]
    low = [half_silu(h).astype(BF16) for h in low]
    lifted = [dot(w3, h) for h in low]
    gates = [jax.nn.sigmoid(v[width : width + 1] + v[width + 1 : width + 2]) for v in lifted]
    total = jnp.zeros((2 * rows, width), F32)
    for members, g, m in zip(chunks, gates, low):
        left = []
        for n, (i, q) in enumerate(members):
            cut = slice(n * LANES, (n + 1) * LANES)
            kept = jnp.where(trow == i, g[:, cut] * keep[q], 0.0)
            left.append(jnp.concatenate(split2(kept), axis=0))
        total = total + lax.dot_general(
            jnp.concatenate(left, axis=1),
            m,
            (((1,), (1,)), ((), ())),
            preferred_element_type=F32,
        )
    weight_rows = {}

    def weigh(picked):
        for k in picked:
            v = half_silu(lifted[k][:width])
            for n, (i, q) in enumerate(chunks[k]):
                cut = slice(n * LANES, (n + 1) * LANES)
                weight_rows[i, q] = jnp.sum(v[:, cut] * ww, axis=0, keepdims=True)

    third = len(chunks) // SPLIT
    message_mean = ((total[:rows] + total[rows:]) * mean_scale).astype(BF16)
    node_pre = node_part + dot(message_mean, w_node[width:, :])
    weigh(range(third))
    node_hidden = half_silu(node_pre * 0.5).astype(BF16)
    change = dot(node_hidden, w_out[...])
    weigh(range(third, len(chunks)))
    feat_out[...] = (x.astype(F32) + change).astype(BF16)
    sums = [jnp.zeros((rows, 1), F32)] * 3
    for q in range(parts):
        weight = jnp.concatenate([weight_rows[i, q] for i in range(rows)], axis=0) * keep[q]
        for c in range(3):
            sums[c] = sums[c] + jnp.sum(unit[q][c] * weight, axis=1, keepdims=True)
    side = jnp.where(lane == 0, sums[0], jnp.where(lane == 1, sums[1], sums[2]))
    coord_out[...] = spot[:3, :rows] + side.T[:3] * mean_scale


def shards(
    node_feat,
    coords,
    pair_table,
    w_tgt,
    w_src,
    w_dist,
    edge_bias,
    w_edge,
    w_gate,
    w_coord,
    w_weight,
    w_node_in,
    w_node_out,
):
    rows, width = node_feat.shape
    edge_parts = lax.axis_size("edge")
    devices = lax.axis_size("blk") * edge_parts
    rounds = pair_table.shape[0]
    mean_scale = 1.0 / ((rounds + 1) * rows * edge_parts - 1)
    vmem = pl.BlockSpec(memory_space=pltpu.VMEM)
    smem = pl.BlockSpec(memory_space=pltpu.SMEM)
    params = pltpu.CompilerParams(vmem_limit_bytes=VMEM_BYTES)
    line = lambda v: v.reshape(1, -1)
    small = (line(w_dist), line(edge_bias), line(w_gate), line(w_weight))
    hold = lambda v: pltpu.with_memory_space_constraint(v, pltpu.HBM)
    sent, lines, table = pl.pallas_call(
        pack_body,
        out_shape=(
            pltpu.VMEM((devices, rows // SLAB + 1, SLAB, width), BF16),
            pltpu.VMEM((8, width), F32),
            pltpu.SMEM(pair_table.shape, pair_table.dtype),
        ),
        in_specs=[vmem] * 2 + [smem] + [vmem] * 4,
        out_specs=(vmem, vmem, smem),
        compiler_params=params,
        name="pack",
    )(*(hold(v) for v in (node_feat, coords, pair_table) + small))
    far = lax.all_to_all(sent, ("blk", "edge"), 0, 0, tiled=True)

    def body(*refs):
        edge_body(*refs, edge_parts=edge_parts, mean_scale=mean_scale)

    return pl.pallas_call(
        body,
        out_shape=(
            jax.ShapeDtypeStruct((rows, width), BF16),
            jax.ShapeDtypeStruct((3, rows), F32),
        ),
        in_specs=[smem] + [vmem] * 8,
        out_specs=(vmem, vmem),
        compiler_params=params,
        name="edges",
    )(
        table,
        far,
        lines,
        w_tgt,
        w_src,
        w_edge,
        w_coord,
        w_node_in,
        w_node_out,
    )


def solution(mesh):
    whole = P()
    placed = (P(("blk", "edge"), None), P(None, ("blk", "edge"))) + (whole,) * 11
    return jax.shard_map(
        shards,
        mesh=mesh,
        in_specs=placed,
        out_specs=(P(("blk", "edge"), None), P(None, ("blk", "edge"))),
        check_vma=False,
    )
```

```python
import jax
import jax.numpy as jnp
from jax import lax
from jax.experimental import pallas as pl
from jax.experimental.pallas import tpu as pltpu
from jax.sharding import PartitionSpec as P

F32 = jnp.float32
BF16 = jnp.bfloat16
LANES = 128
VMEM_BYTES = 24 * 2**20
SPLIT = 2
SLAB = 4


def split2(x):
    hi = x.astype(BF16)
    lo = (x - hi.astype(F32)).astype(BF16)
    return hi, lo


def dot(a, b):
    return jnp.dot(a, b, preferred_element_type=F32)


def half_silu(h):
    return h + h * jnp.tanh(h)


def pack_body(feat, coords, table, w_dist, edge_bias, w_gate, w_weight, *rest):
    weights = rest[: (len(rest) - 3) // 2]
    sent, lines, table_out = rest[len(weights) : len(weights) + 3]
    rows, width = feat.shape
    spot = jnp.concatenate([coords[...].astype(F32), jnp.zeros((SLAB - 3, rows), F32)], axis=0)
    spot = jnp.concatenate([spot, jnp.zeros((SLAB, width - rows), F32)], axis=1)
    slabs = [feat[k : k + SLAB, :] for k in range(0, rows, SLAB)] + [spot.astype(BF16)]
    for k, slab in enumerate(slabs):
        sent[:, k] = jnp.broadcast_to(slab[None], (sent.shape[0],) + slab.shape)
    for k, line in enumerate((w_dist, edge_bias, w_gate, w_weight)):
        lines[k : k + 1, :] = line[...]
    for r in range(table.shape[0]):
        for b in range(table.shape[1]):
            table_out[r, b] = table[r, b]
    for near, weight in zip(rest[len(weights) + 3 :], weights):
        near[...] = weight[...]


def edge_body(
    table,
    lines,
    w_tgt,
    w_src,
    w_edge,
    w_coord,
    w_node,
    w_out,
    *rest,
    edge_parts,
    mean_scale,
):
    far = rest[:edge_parts]
    feat_out, coord_out = rest[edge_parts:]
    rows, width = feat_out.shape
    rounds = table.shape[0]
    block = lax.axis_index("blk")
    last = lax.axis_size("blk") - 1
    blocks = [block] + [table[r, block] for r in range(rounds)]
    places = [(e, last - h) for h in blocks for e in range(edge_parts)]
    slabs = rows // SLAB

    def feats(p):
        return [far[p[0]][p[1], k] for k in range(slabs)]

    def spots_of(p):
        return far[p[0]][p[1], slabs].astype(F32)

    parts = rows * len(places) // LANES
    half = jnp.asarray(0.5, BF16)

    src_t = jnp.concatenate([f for p in places for f in feats(p)], axis=0).T
    spots = jnp.concatenate([spots_of(p)[:, :rows] for p in places], axis=1)

    own = places[0]
    x = jnp.concatenate(feats(own), axis=0)
    w_dist, edge_bias, w_gate, w_weight = (lines[k : k + 1, :] for k in range(4))
    tgt_hi, tgt_lo = split2((dot(x, w_tgt[...]) + edge_bias) * 0.5)
    dist = w_dist * 0.5
    d_hi = dist.astype(BF16).astype(F32)
    urow = lax.broadcasted_iota(jnp.int32, (16, width), 0)
    tail = jnp.where(urow == 1, dist - d_hi, jnp.where(urow < 3, d_hi, 0.0)).astype(BF16)
    a = jnp.concatenate([tgt_hi, tgt_lo, tail], axis=0).T
    src_proj = dot((w_src[...] * half).T, src_t)
    w2 = (w_edge[...] * half).T
    gate_w = w_gate
    g_hi = gate_w.astype(BF16).astype(F32)
    g_rows = jnp.where(urow == 0, g_hi, jnp.where(urow == 1, gate_w - g_hi, 0.0)).astype(BF16)
    w3 = jnp.concatenate([(w_coord[...] * half).T, g_rows], axis=0)
    ww = jnp.broadcast_to(w_weight, (LANES, width)).T
    spot = jnp.concatenate([spots_of(own), jnp.zeros((8 - SLAB, width), F32)], axis=0)
    col = spot.T[:rows]
    node_part = dot(x, w_node[:width, :])

    lane = lax.broadcasted_iota(jnp.int32, (rows, LANES), 1)
    trow = lax.broadcasted_iota(jnp.int32, (rows, LANES), 0)
    unit, keep, r_hi, r_lo = [], [], [], []
    for q in range(parts):
        cut = slice(q * LANES, (q + 1) * LANES)
        off = [col[:, c : c + 1] - spots[c : c + 1, cut] for c in range(3)]
        rad = off[0] * off[0] + off[1] * off[1] + off[2] * off[2]
        scale = 1.0 / (jnp.sqrt(rad) + 1.0)
        unit.append([o * scale for o in off])
        keep.append(jnp.where(lane + q * LANES == trow, 0.0, 1.0))
        hi = rad.astype(BF16).astype(F32)
        r_hi.append(hi)
        r_lo.append(rad - hi)
    lrow = lax.broadcasted_iota(jnp.int32, (16, LANES), 0)
    pairs = [(i, q) for i in range(rows) for q in range(parts)]
    group = 2 if len(pairs) % 2 == 0 else 1
    chunks = [pairs[at : at + group] for at in range(0, len(pairs), group)]
    rights = []
    for members in chunks:
        right = []
        for i, q in members:
            pick = jnp.where(trow == i, 1.0, 0.0).astype(BF16)
            near = jnp.where(
                lrow < 2, r_hi[q][i : i + 1], jnp.where(lrow == 2, r_lo[q][i : i + 1], 0.0)
            ).astype(BF16)
            right.append(jnp.concatenate([pick, pick, near], axis=0))
        rights.append(jnp.concatenate(right, axis=1))
    hidden = []
    for members, right in zip(chunks, rights):
        base = [src_proj[:, q * LANES : (q + 1) * LANES] for _, q in members]
        hidden.append(dot(a, right) + jnp.concatenate(base, axis=1))
    hidden = [half_silu(h).astype(BF16) for h in hidden]
    low = [dot(w2, h) for h in hidden]
    low = [half_silu(h).astype(BF16) for h in low]
    lifted = [dot(w3, h) for h in low]
    gates = [jax.nn.sigmoid(v[width : width + 1] + v[width + 1 : width + 2]) for v in lifted]
    total = jnp.zeros((2 * rows, width), F32)
    for members, g, m in zip(chunks, gates, low):
        left = []
        for n, (i, q) in enumerate(members):
            cut = slice(n * LANES, (n + 1) * LANES)
            kept = jnp.where(trow == i, g[:, cut] * keep[q], 0.0)
            left.append(jnp.concatenate(split2(kept), axis=0))
        total = total + lax.dot_general(
            jnp.concatenate(left, axis=1),
            m,
            (((1,), (1,)), ((), ())),
            preferred_element_type=F32,
        )
    weight_rows = {}

    def weigh(picked):
        for k in picked:
            v = half_silu(lifted[k][:width])
            for n, (i, q) in enumerate(chunks[k]):
                cut = slice(n * LANES, (n + 1) * LANES)
                weight_rows[i, q] = jnp.sum(v[:, cut] * ww, axis=0, keepdims=True)

    third = len(chunks) // SPLIT
    message_mean = ((total[:rows] + total[rows:]) * mean_scale).astype(BF16)
    node_pre = node_part + dot(message_mean, w_node[width:, :])
    weigh(range(third))
    node_hidden = half_silu(node_pre * 0.5).astype(BF16)
    change = dot(node_hidden, w_out[...])
    weigh(range(third, len(chunks)))
    feat_out[...] = (x.astype(F32) + change).astype(BF16)
    sums = [jnp.zeros((rows, 1), F32)] * 3
    for q in range(parts):
        weight = jnp.concatenate([weight_rows[i, q] for i in range(rows)], axis=0) * keep[q]
        for c in range(3):
            sums[c] = sums[c] + jnp.sum(unit[q][c] * weight, axis=1, keepdims=True)
    side = jnp.where(lane == 0, sums[0], jnp.where(lane == 1, sums[1], sums[2]))
    coord_out[...] = spot[:3, :rows] + side.T[:3] * mean_scale


def shards(
    node_feat,
    coords,
    pair_table,
    w_tgt,
    w_src,
    w_dist,
    edge_bias,
    w_edge,
    w_gate,
    w_coord,
    w_weight,
    w_node_in,
    w_node_out,
):
    rows, width = node_feat.shape
    edge_parts = lax.axis_size("edge")
    blocks = lax.axis_size("blk")
    rounds = pair_table.shape[0]
    mean_scale = 1.0 / ((rounds + 1) * rows * edge_parts - 1)
    vmem = pl.BlockSpec(memory_space=pltpu.VMEM)
    smem = pl.BlockSpec(memory_space=pltpu.SMEM)
    params = pltpu.CompilerParams(vmem_limit_bytes=VMEM_BYTES)
    line = lambda v: v.reshape(1, -1)
    small = (line(w_dist), line(edge_bias), line(w_gate), line(w_weight))
    hold = lambda v: pltpu.with_memory_space_constraint(v, pltpu.HBM)
    weights = (w_tgt, w_src, w_edge, w_coord, w_node_in, w_node_out)
    sent, lines, table, *near = pl.pallas_call(
        pack_body,
        out_shape=(
            pltpu.VMEM((blocks, rows // SLAB + 1, SLAB, width), BF16),
            pltpu.VMEM((8, width), F32),
            pltpu.SMEM(pair_table.shape, pair_table.dtype),
        )
        + tuple(pltpu.VMEM(w.shape, w.dtype) for w in weights),
        in_specs=[vmem] * 2 + [smem] + [vmem] * (4 + len(weights)),
        out_specs=(vmem, vmem, smem) + (vmem,) * len(weights),
        compiler_params=params,
        name="pack",
    )(*(hold(v) for v in (node_feat, coords, pair_table) + small + weights))
    order = [list(range(blocks))[::-1]]
    far = [lax.all_to_all(sent, "blk", 0, 0, tiled=True, axis_index_groups=order)]
    for step in range(1, edge_parts):
        ring = [(e, (e + step) % edge_parts) for e in range(edge_parts)]
        far.append(lax.ppermute(far[0], "edge", ring))

    def body(*refs):
        edge_body(*refs, edge_parts=edge_parts, mean_scale=mean_scale)

    return pl.pallas_call(
        body,
        out_shape=(
            jax.ShapeDtypeStruct((rows, width), BF16),
            jax.ShapeDtypeStruct((3, rows), F32),
        ),
        in_specs=[smem] + [vmem] * (7 + edge_parts),
        out_specs=(vmem, vmem),
        compiler_params=params,
        name="edges",
    )(
        table,
        lines,
        *near,
        *far,
    )


def solution(mesh):
    whole = P()
    placed = (P(("blk", "edge"), None), P(None, ("blk", "edge"))) + (whole,) * 11
    return jax.shard_map(
        shards,
        mesh=mesh,
        in_specs=placed,
        out_specs=(P(("blk", "edge"), None), P(None, ("blk", "edge"))),
        check_vma=False,
    )
```

```python
import jax
import jax.numpy as jnp
from jax import lax
from jax.experimental import pallas as pl
from jax.experimental.pallas import tpu as pltpu
from jax.sharding import PartitionSpec as P

F32 = jnp.float32
BF16 = jnp.bfloat16
LANES = 128
VMEM_BYTES = 24 * 2**20
SLAB = 4


def split2(x):
    hi = x.astype(BF16)
    lo = (x - hi.astype(F32)).astype(BF16)
    return hi, lo


def dot(a, b):
    return jnp.dot(a, b, preferred_element_type=F32)


def half_silu(h):
    return h + h * jnp.tanh(h)


def pack_body(feat, coords, table, w_dist, edge_bias, w_gate, w_weight, *rest):
    weights = rest[: (len(rest) - 3) // 2]
    sent, lines, table_out = rest[len(weights) : len(weights) + 3]
    rows, width = feat.shape
    spot = jnp.concatenate([coords[...].astype(F32), jnp.zeros((SLAB - 3, rows), F32)], axis=0)
    spot = jnp.concatenate([spot, jnp.zeros((SLAB, width - rows), F32)], axis=1)
    slabs = [feat[k : k + SLAB, :] for k in range(0, rows, SLAB)] + [spot.astype(BF16)]
    for k, slab in enumerate(slabs):
        sent[:, k] = jnp.broadcast_to(slab[None], (sent.shape[0],) + slab.shape)
    for k, line in enumerate((w_dist, edge_bias, w_gate, w_weight)):
        lines[k : k + 1, :] = line[...]
    for r in range(table.shape[0]):
        for b in range(table.shape[1]):
            table_out[r, b] = table[r, b]
    for near, weight in zip(rest[len(weights) + 3 :], weights):
        near[...] = weight[...]


def half_edges(far, slots, rows, place, keep, mats):
    a, w_src_t, w2, w3, ww = mats
    width = w2.shape[0]
    slabs = rows // SLAB
    sources = rows * len(slots)
    fold = LANES // sources
    groups = rows // fold
    src = [far[p, k] for p in slots for k in range(slabs)]
    src_proj = dot(w_src_t, jnp.concatenate(src * fold, axis=0).T)
    spots = [far[p, slabs].astype(F32)[:, :rows] for p in slots]
    spots = jnp.concatenate(spots * fold, axis=1)
    off = [place[c] - spots[c : c + 1] for c in range(3)]
    rad = off[0] * off[0] + off[1] * off[1] + off[2] * off[2]
    scale = 1.0 / (jnp.sqrt(rad) + 1.0)
    unit = [o * scale for o in off]
    r_hi = rad.astype(BF16).astype(F32)
    r_lo = rad - r_hi
    lrow = lax.broadcasted_iota(jnp.int32, (16, LANES), 0)
    trow = lax.broadcasted_iota(jnp.int32, (rows, LANES), 0)
    upper = groups * (lax.broadcasted_iota(jnp.int32, (rows, LANES), 1) // sources)
    picks = [trow == g + upper for g in range(groups)]
    chunks = [list(range(at, min(at + 2, groups))) for at in range(0, groups, 2)]
    hidden = []
    for members in chunks:
        right = []
        for g in members:
            pick = jnp.where(picks[g], 1.0, 0.0).astype(BF16)
            near = jnp.where(
                lrow < 2, r_hi[g : g + 1], jnp.where(lrow == 2, r_lo[g : g + 1], 0.0)
            ).astype(BF16)
            right.append(jnp.concatenate([pick, pick, near], axis=0))
        base = jnp.concatenate([src_proj] * len(members), axis=1)
        hidden.append(dot(a, jnp.concatenate(right, axis=1)) + base)
    hidden = [half_silu(h).astype(BF16) for h in hidden]
    low = [dot(w2, h) for h in hidden]
    low = [half_silu(h).astype(BF16) for h in low]
    lifted = [dot(w3, h) for h in low]
    gates = [jax.nn.sigmoid(v[width : width + 1] + v[width + 1 : width + 2]) for v in lifted]
    total = jnp.zeros((2 * rows, width), F32)
    for members, gate, m in zip(chunks, gates, low):
        left = []
        for n, g in enumerate(members):
            one = gate[:, n * LANES : (n + 1) * LANES]
            if keep is not None:
                one = one * keep[g : g + 1]
            left.append(jnp.concatenate(split2(jnp.where(picks[g], one, 0.0)), axis=0))
        total = total + lax.dot_general(
            jnp.concatenate(left, axis=1),
            m,
            (((1,), (1,)), ((), ())),
            preferred_element_type=F32,
        )

    def directions():
        weight = []
        for members, v in zip(chunks, lifted):
            v = half_silu(v[:width])
            for n in range(len(members)):
                cut = slice(n * LANES, (n + 1) * LANES)
                weight.append(jnp.sum(v[:, cut] * ww, axis=0, keepdims=True))
        weight = jnp.concatenate(weight, axis=0)
        if keep is not None:
            weight = weight * keep
        return [u * weight for u in unit]

    return total, directions


def near_body(
    table,
    lines,
    w_tgt,
    w_src,
    w_edge,
    w_coord,
    w_node,
    far,
    a_out,
    src_out,
    w2_out,
    w3_out,
    ww_out,
    place_out,
    node_out,
    total_out,
    way_out,
):
    groups = place_out.shape[1]
    rows, width = node_out.shape
    slabs = rows // SLAB
    slots = slots_of(table)
    fold = rows // groups
    sources = LANES // fold
    half = jnp.asarray(0.5, BF16)
    x = jnp.concatenate([far[slots[0], k] for k in range(slabs)], axis=0)
    w_dist, edge_bias, w_gate, w_weight = (lines[k : k + 1, :] for k in range(4))
    tgt_hi, tgt_lo = split2((dot(x, w_tgt[...]) + edge_bias) * 0.5)
    dist = w_dist * 0.5
    d_hi = dist.astype(BF16).astype(F32)
    urow = lax.broadcasted_iota(jnp.int32, (16, width), 0)
    tail = jnp.where(urow == 1, dist - d_hi, jnp.where(urow < 3, d_hi, 0.0)).astype(BF16)
    a = jnp.concatenate([tgt_hi, tgt_lo, tail], axis=0).T
    w_src_t = (w_src[...] * half).T
    w2 = (w_edge[...] * half).T
    g_hi = w_gate.astype(BF16).astype(F32)
    g_rows = jnp.where(urow == 0, g_hi, jnp.where(urow == 1, w_gate - g_hi, 0.0)).astype(BF16)
    w3 = jnp.concatenate([(w_coord[...] * half).T, g_rows], axis=0)
    ww = jnp.broadcast_to(w_weight, (LANES, width)).T
    spot = far[slots[0], slabs].astype(F32)
    col = jnp.concatenate([spot, jnp.zeros((8 - SLAB, width), F32)], axis=0).T
    lane = lax.broadcasted_iota(jnp.int32, (groups, LANES), 1)
    grow = lax.broadcasted_iota(jnp.int32, (groups, LANES), 0)
    place = []
    for c in range(3):
        spread = jnp.broadcast_to(col[:groups, c : c + 1], (groups, LANES))
        for f in range(1, fold):
            there = col[f * groups : (f + 1) * groups, c : c + 1]
            spread = jnp.where(lane >= f * sources, there, spread)
        place.append(spread)
    keep = jnp.where(lane % sources == grow + groups * (lane // sources), 0.0, 1.0)
    a_out[...] = a
    src_out[...] = w_src_t
    w2_out[...] = w2
    w3_out[...] = w3
    ww_out[...] = ww
    node_out[...] = dot(x, w_node[:width, :])
    total, directions = half_edges(
        far, slots, rows, place, keep, (a, w_src_t, w2, w3, ww)
    )
    total_out[...] = total
    for c, way in enumerate(directions()):
        place_out[c] = place[c]
        way_out[c] = way


def slots_of(table):
    block = lax.axis_index("blk")
    last = lax.axis_size("blk") - 1
    return [last - block] + [last - table[r, block] for r in range(table.shape[0])]


def far_body(
    table,
    a_ref,
    src_ref,
    w2_ref,
    w3_ref,
    ww_ref,
    place_ref,
    node_ref,
    total_ref,
    way_ref,
    w_node,
    w_out,
    own,
    *rest,
    mean_scale,
):
    others = rest[:-2]
    feat_out, coord_out = rest[-2:]
    rows, width = feat_out.shape
    groups = place_ref.shape[1]
    fold = rows // groups
    sources = LANES // fold
    slabs = rows // SLAB
    slots = slots_of(table)
    mats = (a_ref[...], src_ref[...], w2_ref[...], w3_ref[...], ww_ref[...])
    place = [place_ref[c] for c in range(3)]
    total = total_ref[...]
    way = [way_ref[c] for c in range(3)]
    pending = []
    for far in others:
        more, directions = half_edges(far, slots, rows, place, None, mats)
        total = total + more
        pending.append(directions)
    message_mean = ((total[:rows] + total[rows:]) * mean_scale).astype(BF16)
    node_pre = node_ref[...] + dot(message_mean, w_node[width:, :])
    node_hidden = half_silu(node_pre * 0.5).astype(BF16)
    change = dot(node_hidden, w_out[...])
    for directions in pending:
        way = [w + more for w, more in zip(way, directions())]
    x = jnp.concatenate([own[slots[0], k] for k in range(slabs)], axis=0)
    feat_out[...] = (x.astype(F32) + change).astype(BF16)
    lane = lax.broadcasted_iota(jnp.int32, (groups, LANES), 1)
    sums = []
    for w in way:
        parts = [
            jnp.sum(jnp.where(lane // sources == f, w, 0.0), axis=1, keepdims=True)
            for f in range(fold)
        ]
        sums.append(jnp.concatenate(parts, axis=0))
    wide = lax.broadcasted_iota(jnp.int32, (rows, LANES), 1)
    side = jnp.where(wide == 0, sums[0], jnp.where(wide == 1, sums[1], sums[2]))
    spot = own[slots[0], slabs].astype(F32)
    coord_out[...] = spot[:3, :rows] + side.T[:3] * mean_scale


def shards(
    node_feat,
    coords,
    pair_table,
    w_tgt,
    w_src,
    w_dist,
    edge_bias,
    w_edge,
    w_gate,
    w_coord,
    w_weight,
    w_node_in,
    w_node_out,
):
    rows, width = node_feat.shape
    edge_parts = lax.axis_size("edge")
    blocks = lax.axis_size("blk")
    rounds = pair_table.shape[0]
    mean_scale = 1.0 / ((rounds + 1) * rows * edge_parts - 1)
    vmem = pl.BlockSpec(memory_space=pltpu.VMEM)
    smem = pl.BlockSpec(memory_space=pltpu.SMEM)
    params = pltpu.CompilerParams(vmem_limit_bytes=VMEM_BYTES)
    line = lambda v: v.reshape(1, -1)
    small = (line(w_dist), line(edge_bias), line(w_gate), line(w_weight))
    hold = lambda v: pltpu.with_memory_space_constraint(v, pltpu.HBM)
    weights = (w_tgt, w_src, w_edge, w_coord, w_node_in, w_node_out)
    sent, lines, table, *near = pl.pallas_call(
        pack_body,
        out_shape=(
            pltpu.VMEM((blocks, rows // SLAB + 1, SLAB, width), BF16),
            pltpu.VMEM((8, width), F32),
            pltpu.SMEM(pair_table.shape, pair_table.dtype),
        )
        + tuple(pltpu.VMEM(w.shape, w.dtype) for w in weights),
        in_specs=[vmem] * 2 + [smem] + [vmem] * (4 + len(weights)),
        out_specs=(vmem, vmem, smem) + (vmem,) * len(weights),
        compiler_params=params,
        name="pack",
    )(*(hold(v) for v in (node_feat, coords, pair_table) + small + weights))
    order = [list(range(blocks))[::-1]]
    far = [lax.all_to_all(sent, "blk", 0, 0, tiled=True, axis_index_groups=order)]
    for step in range(1, edge_parts):
        ring = [(e, (e + step) % edge_parts) for e in range(edge_parts)]
        far.append(lax.ppermute(far[0], "edge", ring))

    w_tgt, w_src, w_edge, w_coord, w_node, w_out = near
    fold = LANES // (rows * (rounds + 1))
    groups = rows // fold
    prepared = pl.pallas_call(
        near_body,
        out_shape=(
            pltpu.VMEM((width, 2 * rows + 16), BF16),
            pltpu.VMEM((width, width), BF16),
            pltpu.VMEM((width, width), BF16),
            pltpu.VMEM((width + 16, width), BF16),
            pltpu.VMEM((width, LANES), F32),
            pltpu.VMEM((3, groups, LANES), F32),
            pltpu.VMEM((rows, width), F32),
            pltpu.VMEM((2 * rows, width), F32),
            pltpu.VMEM((3, groups, LANES), F32),
        ),
        in_specs=[smem] + [vmem] * 7,
        out_specs=(vmem,) * 9,
        compiler_params=params,
        cost_estimate=pl.CostEstimate(
            flops=4 * rows * rows * (rounds + 1) * width * width,
            transcendentals=3 * rows * rows * (rounds + 1) * width,
            bytes_accessed=0,
        ),
        name="near",
    )(table, lines, w_tgt, w_src, w_edge, w_coord, w_node, far[0])

    def body(*refs):
        far_body(*refs, mean_scale=mean_scale)

    return pl.pallas_call(
        body,
        out_shape=(
            jax.ShapeDtypeStruct((rows, width), BF16),
            jax.ShapeDtypeStruct((3, rows), F32),
        ),
        in_specs=[smem] + [vmem] * (11 + edge_parts),
        out_specs=(vmem, vmem),
        compiler_params=params,
        name="far",
    )(table, *prepared, w_node, w_out, *far)


def solution(mesh):
    whole = P()
    placed = (P(("blk", "edge"), None), P(None, ("blk", "edge"))) + (whole,) * 11
    return jax.shard_map(
        shards,
        mesh=mesh,
        in_specs=placed,
        out_specs=(P(("blk", "edge"), None), P(None, ("blk", "edge"))),
        check_vma=False,
    )
```

```python
import jax
import jax.numpy as jnp
from jax import lax
from jax.experimental import pallas as pl
from jax.experimental.pallas import tpu as pltpu
from jax.sharding import PartitionSpec as P

F32 = jnp.float32
BF16 = jnp.bfloat16
LANES = 128
VMEM_BYTES = 24 * 2**20
SLAB = 4


def split2(x):
    hi = x.astype(BF16)
    lo = (x - hi.astype(F32)).astype(BF16)
    return hi, lo


def dot(a, b):
    return jnp.dot(a, b, preferred_element_type=F32)


def half_silu(h):
    return h + h * jnp.tanh(h)


def pack_body(feat, coords, table, w_dist, edge_bias, w_gate, w_weight, *rest):
    weights = rest[: (len(rest) - 3) // 2]
    sent, lines, table_out = rest[len(weights) : len(weights) + 3]
    rows, width = feat.shape
    spot = jnp.concatenate([coords[...].astype(F32), jnp.zeros((SLAB - 3, rows), F32)], axis=0)
    spot = jnp.concatenate([spot, jnp.zeros((SLAB, width - rows), F32)], axis=1)
    slabs = [feat[k : k + SLAB, :] for k in range(0, rows, SLAB)] + [spot.astype(BF16)]
    for k, slab in enumerate(slabs):
        sent[:, k] = jnp.broadcast_to(slab[None], (sent.shape[0],) + slab.shape)
    for k, line in enumerate((w_dist, edge_bias, w_gate, w_weight)):
        lines[k : k + 1, :] = line[...]
    for r in range(table.shape[0]):
        for b in range(table.shape[1]):
            table_out[r, b] = table[r, b]
    for near, weight in zip(rest[len(weights) + 3 :], weights):
        near[...] = weight[...]


def half_edges(far, slots, rows, place, keep, mats):
    a, w_src_t, w2, w3, ww = mats
    width = w2.shape[0]
    slabs = rows // SLAB
    sources = rows * len(slots)
    fold = LANES // sources
    groups = rows // fold
    src = [far[p, k] for p in slots for k in range(slabs)]
    src_proj = dot(w_src_t, jnp.concatenate(src * fold, axis=0).T)
    spots = [far[p, slabs].astype(F32)[:, :rows] for p in slots]
    spots = jnp.concatenate(spots * fold, axis=1)
    off = [place[c] - spots[c : c + 1] for c in range(3)]
    rad = off[0] * off[0] + off[1] * off[1] + off[2] * off[2]
    scale = 1.0 / (jnp.sqrt(rad) + 1.0)
    unit = [o * scale for o in off]
    r_hi = rad.astype(BF16).astype(F32)
    r_lo = rad - r_hi
    lrow = lax.broadcasted_iota(jnp.int32, (16, LANES), 0)
    trow = lax.broadcasted_iota(jnp.int32, (rows, LANES), 0)
    upper = groups * (lax.broadcasted_iota(jnp.int32, (rows, LANES), 1) // sources)
    picks = [trow == g + upper for g in range(groups)]
    chunks = [list(range(at, min(at + 2, groups))) for at in range(0, groups, 2)]
    hidden = []
    for members in chunks:
        right = []
        for g in members:
            pick = jnp.where(picks[g], 1.0, 0.0).astype(BF16)
            near = jnp.where(
                lrow < 2, r_hi[g : g + 1], jnp.where(lrow == 2, r_lo[g : g + 1], 0.0)
            ).astype(BF16)
            right.append(jnp.concatenate([pick, pick, near], axis=0))
        base = jnp.concatenate([src_proj] * len(members), axis=1)
        hidden.append(dot(a, jnp.concatenate(right, axis=1)) + base)
    hidden = [half_silu(h).astype(BF16) for h in hidden]
    low = [dot(w2, h) for h in hidden]
    low = [half_silu(h).astype(BF16) for h in low]
    lifted = [dot(w3, h) for h in low]
    gates = [jax.nn.sigmoid(v[:1] + v[1:2]) for v in lifted]
    left = []
    for members, gate in zip(chunks, gates):
        for n, g in enumerate(members):
            one = gate[:, n * LANES : (n + 1) * LANES]
            if keep is not None:
                one = one * keep[g : g + 1]
            left.append(jnp.concatenate(split2(jnp.where(picks[g], one, 0.0)), axis=0))
    total = lax.dot_general(
        jnp.concatenate(left, axis=1),
        jnp.concatenate(low, axis=1),
        (((1,), (1,)), ((), ())),
        preferred_element_type=F32,
    )

    def directions():
        weight = []
        for members, v in zip(chunks, lifted):
            v = half_silu(v[16:])
            for n in range(len(members)):
                cut = slice(n * LANES, (n + 1) * LANES)
                weight.append(jnp.sum(v[:, cut] * ww, axis=0, keepdims=True))
        weight = jnp.concatenate(weight, axis=0)
        if keep is not None:
            weight = weight * keep
        return [u * weight for u in unit]

    return total, directions


def near_body(
    table,
    lines,
    w_tgt,
    w_src,
    w_edge,
    w_coord,
    w_node,
    far,
    a_out,
    src_out,
    w2_out,
    w3_out,
    ww_out,
    place_out,
    node_out,
    total_out,
    way_out,
):
    groups = place_out.shape[1]
    rows, width = node_out.shape
    slabs = rows // SLAB
    slots = slots_of(table)
    fold = rows // groups
    sources = LANES // fold
    half = jnp.asarray(0.5, BF16)
    x = jnp.concatenate([far[slots[0], k] for k in range(slabs)], axis=0)
    w_dist, edge_bias, w_gate, w_weight = (lines[k : k + 1, :] for k in range(4))
    tgt_hi, tgt_lo = split2((dot(x, w_tgt[...]) + edge_bias) * 0.5)
    dist = w_dist * 0.5
    d_hi = dist.astype(BF16).astype(F32)
    urow = lax.broadcasted_iota(jnp.int32, (16, width), 0)
    tail = jnp.where(urow == 1, dist - d_hi, jnp.where(urow < 3, d_hi, 0.0)).astype(BF16)
    a = jnp.concatenate([tgt_hi, tgt_lo, tail], axis=0).T
    w_src_t = (w_src[...] * half).T
    w2 = (w_edge[...] * half).T
    g_hi = w_gate.astype(BF16).astype(F32)
    g_rows = jnp.where(urow == 0, g_hi, jnp.where(urow == 1, w_gate - g_hi, 0.0)).astype(BF16)
    w3 = jnp.concatenate([g_rows, (w_coord[...] * half).T], axis=0)
    ww = jnp.broadcast_to(w_weight, (LANES, width)).T
    spot = far[slots[0], slabs].astype(F32)
    col = jnp.concatenate([spot, jnp.zeros((8 - SLAB, width), F32)], axis=0).T
    lane = lax.broadcasted_iota(jnp.int32, (groups, LANES), 1)
    grow = lax.broadcasted_iota(jnp.int32, (groups, LANES), 0)
    place = []
    for c in range(3):
        spread = jnp.broadcast_to(col[:groups, c : c + 1], (groups, LANES))
        for f in range(1, fold):
            there = col[f * groups : (f + 1) * groups, c : c + 1]
            spread = jnp.where(lane >= f * sources, there, spread)
        place.append(spread)
    keep = jnp.where(lane % sources == grow + groups * (lane // sources), 0.0, 1.0)
    a_out[...] = a
    src_out[...] = w_src_t
    w2_out[...] = w2
    w3_out[...] = w3
    ww_out[...] = ww
    node_out[...] = dot(x, w_node[:width, :])
    total, directions = half_edges(
        far, slots, rows, place, keep, (a, w_src_t, w2, w3, ww)
    )
    total_out[...] = total
    for c, way in enumerate(directions()):
        place_out[c] = place[c]
        way_out[c] = way


def slots_of(table):
    block = lax.axis_index("blk")
    last = lax.axis_size("blk") - 1
    return [last - block] + [last - table[r, block] for r in range(table.shape[0])]


def far_body(
    table,
    a_ref,
    src_ref,
    w2_ref,
    w3_ref,
    ww_ref,
    place_ref,
    node_ref,
    total_ref,
    way_ref,
    w_node,
    w_out,
    own,
    *rest,
    mean_scale,
):
    others = rest[:-2]
    feat_out, coord_out = rest[-2:]
    rows, width = feat_out.shape
    groups = place_ref.shape[1]
    fold = rows // groups
    sources = LANES // fold
    slabs = rows // SLAB
    slots = slots_of(table)
    mats = (a_ref[...], src_ref[...], w2_ref[...], w3_ref[...], ww_ref[...])
    place = [place_ref[c] for c in range(3)]
    total = total_ref[...]
    way = [way_ref[c] for c in range(3)]
    pending = []
    for far in others:
        more, directions = half_edges(far, slots, rows, place, None, mats)
        total = total + more
        pending.append(directions)
    message_mean = ((total[:rows] + total[rows:]) * mean_scale).astype(BF16)
    node_pre = node_ref[...] + dot(message_mean, w_node[width:, :])
    node_hidden = half_silu(node_pre * 0.5).astype(BF16)
    change = dot(node_hidden, w_out[...])
    for directions in pending:
        way = [w + more for w, more in zip(way, directions())]
    x = jnp.concatenate([own[slots[0], k] for k in range(slabs)], axis=0)
    feat_out[...] = (x.astype(F32) + change).astype(BF16)
    lane = lax.broadcasted_iota(jnp.int32, (groups, LANES), 1)
    sums = []
    for w in way:
        parts = [
            jnp.sum(jnp.where(lane // sources == f, w, 0.0), axis=1, keepdims=True)
            for f in range(fold)
        ]
        sums.append(jnp.concatenate(parts, axis=0))
    wide = lax.broadcasted_iota(jnp.int32, (rows, LANES), 1)
    side = jnp.where(wide == 0, sums[0], jnp.where(wide == 1, sums[1], sums[2]))
    spot = own[slots[0], slabs].astype(F32)
    coord_out[...] = spot[:3, :rows] + side.T[:3] * mean_scale


def shards(
    node_feat,
    coords,
    pair_table,
    w_tgt,
    w_src,
    w_dist,
    edge_bias,
    w_edge,
    w_gate,
    w_coord,
    w_weight,
    w_node_in,
    w_node_out,
):
    rows, width = node_feat.shape
    edge_parts = lax.axis_size("edge")
    blocks = lax.axis_size("blk")
    rounds = pair_table.shape[0]
    mean_scale = 1.0 / ((rounds + 1) * rows * edge_parts - 1)
    vmem = pl.BlockSpec(memory_space=pltpu.VMEM)
    smem = pl.BlockSpec(memory_space=pltpu.SMEM)
    params = pltpu.CompilerParams(vmem_limit_bytes=VMEM_BYTES)
    line = lambda v: v.reshape(1, -1)
    small = (line(w_dist), line(edge_bias), line(w_gate), line(w_weight))
    hold = lambda v: pltpu.with_memory_space_constraint(v, pltpu.HBM)
    weights = (w_tgt, w_src, w_edge, w_coord, w_node_in, w_node_out)
    sent, lines, table, *near = pl.pallas_call(
        pack_body,
        out_shape=(
            pltpu.VMEM((blocks, rows // SLAB + 1, SLAB, width), BF16),
            pltpu.VMEM((8, width), F32),
            pltpu.SMEM(pair_table.shape, pair_table.dtype),
        )
        + tuple(pltpu.VMEM(w.shape, w.dtype) for w in weights),
        in_specs=[vmem] * 2 + [smem] + [vmem] * (4 + len(weights)),
        out_specs=(vmem, vmem, smem) + (vmem,) * len(weights),
        compiler_params=params,
        name="pack",
    )(*(hold(v) for v in (node_feat, coords, pair_table) + small + weights))
    order = [list(range(blocks))[::-1]]
    far = [lax.all_to_all(sent, "blk", 0, 0, tiled=True, axis_index_groups=order)]
    for step in range(1, edge_parts):
        ring = [(e, (e + step) % edge_parts) for e in range(edge_parts)]
        far.append(lax.ppermute(far[0], "edge", ring))

    w_tgt, w_src, w_edge, w_coord, w_node, w_out = near
    fold = LANES // (rows * (rounds + 1))
    groups = rows // fold
    prepared = pl.pallas_call(
        near_body,
        out_shape=(
            pltpu.VMEM((width, 2 * rows + 16), BF16),
            pltpu.VMEM((width, width), BF16),
            pltpu.VMEM((width, width), BF16),
            pltpu.VMEM((width + 16, width), BF16),
            pltpu.VMEM((width, LANES), F32),
            pltpu.VMEM((3, groups, LANES), F32),
            pltpu.VMEM((rows, width), F32),
            pltpu.VMEM((2 * rows, width), F32),
            pltpu.VMEM((3, groups, LANES), F32),
        ),
        in_specs=[smem] + [vmem] * 7,
        out_specs=(vmem,) * 9,
        compiler_params=params,
        cost_estimate=pl.CostEstimate(
            flops=4 * rows * rows * (rounds + 1) * width * width,
            transcendentals=3 * rows * rows * (rounds + 1) * width,
            bytes_accessed=0,
        ),
        name="near",
    )(table, lines, w_tgt, w_src, w_edge, w_coord, w_node, far[0])

    def body(*refs):
        far_body(*refs, mean_scale=mean_scale)

    return pl.pallas_call(
        body,
        out_shape=(
            jax.ShapeDtypeStruct((rows, width), BF16),
            jax.ShapeDtypeStruct((3, rows), F32),
        ),
        in_specs=[smem] + [vmem] * (11 + edge_parts),
        out_specs=(vmem, vmem),
        compiler_params=params,
        name="far",
    )(table, *prepared, w_node, w_out, *far)


def solution(mesh):
    whole = P()
    placed = (P(("blk", "edge"), None), P(None, ("blk", "edge"))) + (whole,) * 11
    return jax.shard_map(
        shards,
        mesh=mesh,
        in_specs=placed,
        out_specs=(P(("blk", "edge"), None), P(None, ("blk", "edge"))),
        check_vma=False,
    )
```

```python
import jax
import jax.numpy as jnp
from jax import lax
from jax.experimental import pallas as pl
from jax.experimental.pallas import tpu as pltpu
from jax.sharding import PartitionSpec as P

F32 = jnp.float32
BF16 = jnp.bfloat16
LANES = 128
VMEM_BYTES = 24 * 2**20
SLAB = 4


def split2(x):
    hi = x.astype(BF16)
    lo = (x - hi.astype(F32)).astype(BF16)
    return hi, lo


def dot(a, b):
    return jnp.dot(a, b, preferred_element_type=F32)


def half_silu(h):
    return h + h * jnp.tanh(h)


def pack_body(feat, coords, table, w_dist, edge_bias, w_gate, w_weight, *rest):
    weights = rest[: (len(rest) - 3) // 2]
    sent, lines, table_out = rest[len(weights) : len(weights) + 3]
    rows, width = feat.shape
    spot = jnp.concatenate([coords[...].astype(F32), jnp.zeros((SLAB - 3, rows), F32)], axis=0)
    spot = jnp.concatenate([spot, jnp.zeros((SLAB, width - rows), F32)], axis=1)
    slabs = [feat[k : k + SLAB, :] for k in range(0, rows, SLAB)] + [spot.astype(BF16)]
    for k, slab in enumerate(slabs):
        sent[:, k] = jnp.broadcast_to(slab[None], (sent.shape[0],) + slab.shape)
    for k, line in enumerate((w_dist, edge_bias, w_gate, w_weight)):
        lines[k : k + 1, :] = line[...]
    for r in range(table.shape[0]):
        for b in range(table.shape[1]):
            table_out[r, b] = table[r, b]
    for near, weight in zip(rest[len(weights) + 3 :], weights):
        near[...] = weight[...]


def half_edges(far, slots, rows, place, keep, mats):
    a, w_src_t, w2, w3, ww = mats
    width = w2.shape[0]
    slabs = rows // SLAB
    sources = rows * len(slots)
    fold = LANES // sources
    groups = rows // fold
    src = [far[p, k] for p in slots for k in range(slabs)]
    src_proj = dot(w_src_t, jnp.concatenate(src * fold, axis=0).T)
    spots = [far[p, slabs].astype(F32)[:, :rows] for p in slots]
    spots = jnp.concatenate(spots * fold, axis=1)
    off = [place[c] - spots[c : c + 1] for c in range(3)]
    rad = off[0] * off[0] + off[1] * off[1] + off[2] * off[2]
    scale = 1.0 / (jnp.sqrt(rad) + 1.0)
    unit = [o * scale for o in off]
    r_hi = rad.astype(BF16).astype(F32)
    r_lo = rad - r_hi
    lrow = lax.broadcasted_iota(jnp.int32, (16, LANES), 0)
    trow = lax.broadcasted_iota(jnp.int32, (rows, LANES), 0)
    upper = groups * (lax.broadcasted_iota(jnp.int32, (rows, LANES), 1) // sources)
    picks = [trow == g + upper for g in range(groups)]
    chunks = [list(range(at, min(at + 2, groups))) for at in range(0, groups, 2)]
    hidden = []
    for members in chunks:
        right = []
        for g in members:
            pick = jnp.where(picks[g], 1.0, 0.0).astype(BF16)
            near = jnp.where(
                lrow < 2, r_hi[g : g + 1], jnp.where(lrow == 2, r_lo[g : g + 1], 0.0)
            ).astype(BF16)
            right.append(jnp.concatenate([pick, pick, near], axis=0))
        base = jnp.concatenate([src_proj] * len(members), axis=1)
        hidden.append(dot(a, jnp.concatenate(right, axis=1)) + base)
    hidden = [half_silu(h).astype(BF16) for h in hidden]
    low = [dot(w2, h) for h in hidden]
    low = [half_silu(h).astype(BF16) for h in low]
    lifted = [dot(w3, h) for h in low]
    gates = [0.5 + 0.5 * jnp.tanh((v[:1] + v[1:2]) * 0.5) for v in lifted]
    left = []
    for members, gate in zip(chunks, gates):
        for n, g in enumerate(members):
            one = gate[:, n * LANES : (n + 1) * LANES]
            if keep is not None:
                one = one * keep[g : g + 1]
            left.append(jnp.concatenate(split2(jnp.where(picks[g], one, 0.0)), axis=0))
    total = lax.dot_general(
        jnp.concatenate(left, axis=1),
        jnp.concatenate(low, axis=1),
        (((1,), (1,)), ((), ())),
        preferred_element_type=F32,
    )

    def directions():
        weight = []
        for members, v in zip(chunks, lifted):
            v = half_silu(v[16:])
            for n in range(len(members)):
                cut = slice(n * LANES, (n + 1) * LANES)
                weight.append(jnp.sum(v[:, cut] * ww, axis=0, keepdims=True))
        weight = jnp.concatenate(weight, axis=0)
        if keep is not None:
            weight = weight * keep
        return [u * weight for u in unit]

    return total, directions


def near_body(
    table,
    lines,
    w_tgt,
    w_src,
    w_edge,
    w_coord,
    w_node,
    far,
    a_out,
    src_out,
    w2_out,
    w3_out,
    ww_out,
    place_out,
    node_out,
    total_out,
    way_out,
):
    groups = place_out.shape[1]
    rows, width = node_out.shape
    slabs = rows // SLAB
    slots = slots_of(table)
    fold = rows // groups
    sources = LANES // fold
    half = jnp.asarray(0.5, BF16)
    x = jnp.concatenate([far[slots[0], k] for k in range(slabs)], axis=0)
    w_dist, edge_bias, w_gate, w_weight = (lines[k : k + 1, :] for k in range(4))
    tgt_hi, tgt_lo = split2((dot(x, w_tgt[...]) + edge_bias) * 0.5)
    dist = w_dist * 0.5
    d_hi = dist.astype(BF16).astype(F32)
    urow = lax.broadcasted_iota(jnp.int32, (16, width), 0)
    tail = jnp.where(urow == 1, dist - d_hi, jnp.where(urow < 3, d_hi, 0.0)).astype(BF16)
    a = jnp.concatenate([tgt_hi, tgt_lo, tail], axis=0).T
    w_src_t = (w_src[...] * half).T
    w2 = (w_edge[...] * half).T
    g_hi = w_gate.astype(BF16).astype(F32)
    g_rows = jnp.where(urow == 0, g_hi, jnp.where(urow == 1, w_gate - g_hi, 0.0)).astype(BF16)
    w3 = jnp.concatenate([g_rows, (w_coord[...] * half).T], axis=0)
    ww = jnp.broadcast_to(w_weight, (LANES, width)).T
    spot = far[slots[0], slabs].astype(F32)
    col = jnp.concatenate([spot, jnp.zeros((8 - SLAB, width), F32)], axis=0).T
    lane = lax.broadcasted_iota(jnp.int32, (groups, LANES), 1)
    grow = lax.broadcasted_iota(jnp.int32, (groups, LANES), 0)
    place = []
    for c in range(3):
        spread = jnp.broadcast_to(col[:groups, c : c + 1], (groups, LANES))
        for f in range(1, fold):
            there = col[f * groups : (f + 1) * groups, c : c + 1]
            spread = jnp.where(lane >= f * sources, there, spread)
        place.append(spread)
    keep = jnp.where(lane % sources == grow + groups * (lane // sources), 0.0, 1.0)
    a_out[...] = a
    src_out[...] = w_src_t
    w2_out[...] = w2
    w3_out[...] = w3
    ww_out[...] = ww
    node_out[...] = dot(x, w_node[:width, :])
    total, directions = half_edges(
        far, slots, rows, place, keep, (a, w_src_t, w2, w3, ww)
    )
    total_out[...] = total
    for c, way in enumerate(directions()):
        place_out[c] = place[c]
        way_out[c] = way


def slots_of(table):
    block = lax.axis_index("blk")
    last = lax.axis_size("blk") - 1
    return [last - block] + [last - table[r, block] for r in range(table.shape[0])]


def far_body(
    table,
    a_ref,
    src_ref,
    w2_ref,
    w3_ref,
    ww_ref,
    place_ref,
    node_ref,
    total_ref,
    way_ref,
    w_node,
    w_out,
    own,
    *rest,
    mean_scale,
):
    others = rest[:-2]
    feat_out, coord_out = rest[-2:]
    rows, width = feat_out.shape
    groups = place_ref.shape[1]
    fold = rows // groups
    sources = LANES // fold
    slabs = rows // SLAB
    slots = slots_of(table)
    mats = (a_ref[...], src_ref[...], w2_ref[...], w3_ref[...], ww_ref[...])
    place = [place_ref[c] for c in range(3)]
    total = total_ref[...]
    way = [way_ref[c] for c in range(3)]
    pending = []
    for far in others:
        more, directions = half_edges(far, slots, rows, place, None, mats)
        total = total + more
        pending.append(directions)
    message_mean = ((total[:rows] + total[rows:]) * mean_scale).astype(BF16)
    node_pre = node_ref[...] + dot(message_mean, w_node[width:, :])
    node_hidden = half_silu(node_pre * 0.5).astype(BF16)
    change = dot(node_hidden, w_out[...])
    for directions in pending:
        way = [w + more for w, more in zip(way, directions())]
    x = jnp.concatenate([own[slots[0], k] for k in range(slabs)], axis=0)
    feat_out[...] = (x.astype(F32) + change).astype(BF16)
    lane = lax.broadcasted_iota(jnp.int32, (groups, LANES), 1)
    sums = []
    for w in way:
        parts = [
            jnp.sum(jnp.where(lane // sources == f, w, 0.0), axis=1, keepdims=True)
            for f in range(fold)
        ]
        sums.append(jnp.concatenate(parts, axis=0))
    wide = lax.broadcasted_iota(jnp.int32, (rows, LANES), 1)
    side = jnp.where(wide == 0, sums[0], jnp.where(wide == 1, sums[1], sums[2]))
    spot = own[slots[0], slabs].astype(F32)
    coord_out[...] = spot[:3, :rows] + side.T[:3] * mean_scale


def shards(
    node_feat,
    coords,
    pair_table,
    w_tgt,
    w_src,
    w_dist,
    edge_bias,
    w_edge,
    w_gate,
    w_coord,
    w_weight,
    w_node_in,
    w_node_out,
):
    rows, width = node_feat.shape
    edge_parts = lax.axis_size("edge")
    blocks = lax.axis_size("blk")
    rounds = pair_table.shape[0]
    mean_scale = 1.0 / ((rounds + 1) * rows * edge_parts - 1)
    vmem = pl.BlockSpec(memory_space=pltpu.VMEM)
    smem = pl.BlockSpec(memory_space=pltpu.SMEM)
    params = pltpu.CompilerParams(vmem_limit_bytes=VMEM_BYTES)
    line = lambda v: v.reshape(1, -1)
    small = (line(w_dist), line(edge_bias), line(w_gate), line(w_weight))
    hold = lambda v: pltpu.with_memory_space_constraint(v, pltpu.HBM)
    weights = (w_tgt, w_src, w_edge, w_coord, w_node_in, w_node_out)
    sent, lines, table, *near = pl.pallas_call(
        pack_body,
        out_shape=(
            pltpu.VMEM((blocks, rows // SLAB + 1, SLAB, width), BF16),
            pltpu.VMEM((8, width), F32),
            pltpu.SMEM(pair_table.shape, pair_table.dtype),
        )
        + tuple(pltpu.VMEM(w.shape, w.dtype) for w in weights),
        in_specs=[vmem] * 2 + [smem] + [vmem] * (4 + len(weights)),
        out_specs=(vmem, vmem, smem) + (vmem,) * len(weights),
        compiler_params=params,
        name="pack",
    )(*(hold(v) for v in (node_feat, coords, pair_table) + small + weights))
    order = [list(range(blocks))[::-1]]
    far = [lax.all_to_all(sent, "blk", 0, 0, tiled=True, axis_index_groups=order)]
    for step in range(1, edge_parts):
        ring = [(e, (e + step) % edge_parts) for e in range(edge_parts)]
        far.append(lax.ppermute(far[0], "edge", ring))

    w_tgt, w_src, w_edge, w_coord, w_node, w_out = near
    fold = LANES // (rows * (rounds + 1))
    groups = rows // fold
    prepared = pl.pallas_call(
        near_body,
        out_shape=(
            pltpu.VMEM((width, 2 * rows + 16), BF16),
            pltpu.VMEM((width, width), BF16),
            pltpu.VMEM((width, width), BF16),
            pltpu.VMEM((width + 16, width), BF16),
            pltpu.VMEM((width, LANES), F32),
            pltpu.VMEM((3, groups, LANES), F32),
            pltpu.VMEM((rows, width), F32),
            pltpu.VMEM((2 * rows, width), F32),
            pltpu.VMEM((3, groups, LANES), F32),
        ),
        in_specs=[smem] + [vmem] * 7,
        out_specs=(vmem,) * 9,
        compiler_params=params,
        cost_estimate=pl.CostEstimate(
            flops=4 * rows * rows * (rounds + 1) * width * width,
            transcendentals=3 * rows * rows * (rounds + 1) * width,
            bytes_accessed=0,
        ),
        name="near",
    )(table, lines, w_tgt, w_src, w_edge, w_coord, w_node, far[0])

    def body(*refs):
        far_body(*refs, mean_scale=mean_scale)

    return pl.pallas_call(
        body,
        out_shape=(
            jax.ShapeDtypeStruct((rows, width), BF16),
            jax.ShapeDtypeStruct((3, rows), F32),
        ),
        in_specs=[smem] + [vmem] * (11 + edge_parts),
        out_specs=(vmem, vmem),
        compiler_params=params,
        name="far",
    )(table, *prepared, w_node, w_out, *far)


def solution(mesh):
    whole = P()
    placed = (P(("blk", "edge"), None), P(None, ("blk", "edge"))) + (whole,) * 11
    return jax.shard_map(
        shards,
        mesh=mesh,
        in_specs=placed,
        out_specs=(P(("blk", "edge"), None), P(None, ("blk", "edge"))),
        check_vma=False,
    )
```

```python
import jax
import jax.numpy as jnp
from jax import lax
from jax.experimental import pallas as pl
from jax.experimental.pallas import tpu as pltpu
from jax.sharding import PartitionSpec as P

F32 = jnp.float32
BF16 = jnp.bfloat16
LANES = 128
VMEM_BYTES = 24 * 2**20
SLAB = 4


def split2(x):
    hi = x.astype(BF16)
    lo = (x - hi.astype(F32)).astype(BF16)
    return hi, lo


def dot(a, b):
    return jnp.dot(a, b, preferred_element_type=F32)


def half_silu(h):
    return h + h * jnp.tanh(h)


def pack_body(feat, coords, table, w_dist, edge_bias, w_gate, w_weight, *rest):
    weights = rest[: (len(rest) - 3) // 2]
    sent, lines, table_out = rest[len(weights) : len(weights) + 3]
    rows, width = feat.shape
    spot = jnp.concatenate([coords[...].astype(F32), jnp.zeros((SLAB - 3, rows), F32)], axis=0)
    spot = jnp.concatenate([spot, jnp.zeros((SLAB, width - rows), F32)], axis=1)
    slabs = [feat[k : k + SLAB, :] for k in range(0, rows, SLAB)] + [spot.astype(BF16)]
    for k, slab in enumerate(slabs):
        sent[:, k] = jnp.broadcast_to(slab[None], (sent.shape[0],) + slab.shape)
    for k, line in enumerate((w_dist, edge_bias, w_gate, w_weight)):
        lines[k : k + 1, :] = line[...]
    for r in range(table.shape[0]):
        for b in range(table.shape[1]):
            table_out[r, b] = table[r, b]
    for near, weight in zip(rest[len(weights) + 3 :], weights):
        near[...] = weight[...]


def half_edges(far, slots, rows, place, keep, mats):
    a, w_src_t, w2, w3, ww = mats
    width = w2.shape[0]
    slabs = rows // SLAB
    sources = rows * len(slots)
    fold = LANES // sources
    groups = rows // fold
    src = [far[p, k] for p in slots for k in range(slabs)]
    src_proj = dot(w_src_t, jnp.concatenate(src * fold, axis=0).T)
    spots = [far[p, slabs].astype(F32)[:, :rows] for p in slots]
    spots = jnp.concatenate(spots * fold, axis=1)
    off = [place[c] - spots[c : c + 1] for c in range(3)]
    rad = off[0] * off[0] + off[1] * off[1] + off[2] * off[2]
    scale = 1.0 / (jnp.sqrt(rad) + 1.0)
    unit = [o * scale for o in off]
    r_hi = rad.astype(BF16).astype(F32)
    r_lo = rad - r_hi
    lrow = lax.broadcasted_iota(jnp.int32, (16, LANES), 0)
    trow = lax.broadcasted_iota(jnp.int32, (rows, LANES), 0)
    upper = groups * (lax.broadcasted_iota(jnp.int32, (rows, LANES), 1) // sources)
    picks = [trow == g + upper for g in range(groups)]
    chunks = [list(range(at, min(at + 2, groups))) for at in range(0, groups, 2)]
    hidden = []
    for members in chunks:
        right = []
        for g in members:
            pick = jnp.where(picks[g], 1.0, 0.0).astype(BF16)
            near = jnp.where(
                lrow < 2, r_hi[g : g + 1], jnp.where(lrow == 2, r_lo[g : g + 1], 0.0)
            ).astype(BF16)
            right.append(jnp.concatenate([pick, pick, near], axis=0))
        base = jnp.concatenate([src_proj] * len(members), axis=1)
        hidden.append(dot(a, jnp.concatenate(right, axis=1)) + base)
    hidden = [half_silu(h).astype(BF16) for h in hidden]
    low = [dot(w2, h) for h in hidden]
    low = [half_silu(h).astype(BF16) for h in low]
    lifted = [dot(w3, h) for h in low]
    gates = [0.5 + 0.5 * jnp.tanh((v[:1] + v[1:2]) * 0.5) for v in lifted]
    left = []
    for members, gate in zip(chunks, gates):
        for n, g in enumerate(members):
            one = gate[:, n * LANES : (n + 1) * LANES]
            if keep is not None:
                one = one * keep[g : g + 1]
            left.append(jnp.concatenate(split2(jnp.where(picks[g], one, 0.0)), axis=0))
    total = lax.dot_general(
        jnp.concatenate(left, axis=1),
        jnp.concatenate(low, axis=1),
        (((1,), (1,)), ((), ())),
        preferred_element_type=F32,
    )

    def directions():
        weight = []
        for members, v in zip(chunks, lifted):
            v = half_silu(v[16:])
            for n in range(len(members)):
                cut = slice(n * LANES, (n + 1) * LANES)
                weight.append(jnp.sum(v[:, cut] * ww, axis=0, keepdims=True))
        weight = jnp.concatenate(weight, axis=0)
        if keep is not None:
            weight = weight * keep
        return [u * weight for u in unit]

    return total, directions


def near_body(
    table,
    lines,
    w_tgt,
    w_src,
    w_edge,
    w_coord,
    w_node,
    far,
    a_out,
    src_out,
    w2_out,
    w3_out,
    ww_out,
    place_out,
    node_out,
    total_out,
    way_out,
):
    groups = place_out.shape[1]
    rows, width = node_out.shape
    slabs = rows // SLAB
    slots = slots_of(table)
    fold = rows // groups
    sources = LANES // fold
    half = jnp.asarray(0.5, BF16)
    x = jnp.concatenate([far[slots[0], k] for k in range(slabs)], axis=0)
    w_dist, edge_bias, w_gate, w_weight = (lines[k : k + 1, :] for k in range(4))
    tgt_hi, tgt_lo = split2((dot(x, w_tgt[...]) + edge_bias) * 0.5)
    dist = w_dist * 0.5
    d_hi = dist.astype(BF16).astype(F32)
    urow = lax.broadcasted_iota(jnp.int32, (16, width), 0)
    tail = jnp.where(urow == 1, dist - d_hi, jnp.where(urow < 3, d_hi, 0.0)).astype(BF16)
    a = jnp.concatenate([tgt_hi, tgt_lo, tail], axis=0).T
    w_src_t = (w_src[...] * half).T
    w2 = (w_edge[...] * half).T
    g_hi = w_gate.astype(BF16).astype(F32)
    g_rows = jnp.where(urow == 0, g_hi, jnp.where(urow == 1, w_gate - g_hi, 0.0)).astype(BF16)
    w3 = jnp.concatenate([g_rows, (w_coord[...] * half).T], axis=0)
    ww = jnp.broadcast_to(w_weight, (LANES, width)).T
    spot = far[slots[0], slabs].astype(F32)
    col = jnp.concatenate([spot, jnp.zeros((8 - SLAB, width), F32)], axis=0).T
    lane = lax.broadcasted_iota(jnp.int32, (groups, LANES), 1)
    grow = lax.broadcasted_iota(jnp.int32, (groups, LANES), 0)
    place = []
    for c in range(3):
        spread = jnp.broadcast_to(col[:groups, c : c + 1], (groups, LANES))
        for f in range(1, fold):
            there = col[f * groups : (f + 1) * groups, c : c + 1]
            spread = jnp.where(lane >= f * sources, there, spread)
        place.append(spread)
    keep = jnp.where(lane % sources == grow + groups * (lane // sources), 0.0, 1.0)
    a_out[...] = a
    src_out[...] = w_src_t
    w2_out[...] = w2
    w3_out[...] = w3
    ww_out[...] = ww
    node_out[...] = dot(x, w_node[:width, :])
    total, directions = half_edges(
        far, slots, rows, place, keep, (a, w_src_t, w2, w3, ww)
    )
    total_out[...] = total
    for c, way in enumerate(directions()):
        place_out[c] = place[c]
        way_out[c] = way


def slots_of(table):
    block = lax.axis_index("blk")
    last = lax.axis_size("blk") - 1
    homes = [block] + [table[r, block] for r in range(table.shape[0])]
    return [jnp.where(h == last, 0, h + 1) for h in homes]


def far_body(
    table,
    a_ref,
    src_ref,
    w2_ref,
    w3_ref,
    ww_ref,
    place_ref,
    node_ref,
    total_ref,
    way_ref,
    w_node,
    w_out,
    own,
    *rest,
    mean_scale,
):
    others = rest[:-2]
    feat_out, coord_out = rest[-2:]
    rows, width = feat_out.shape
    groups = place_ref.shape[1]
    fold = rows // groups
    sources = LANES // fold
    slabs = rows // SLAB
    slots = slots_of(table)
    mats = (a_ref[...], src_ref[...], w2_ref[...], w3_ref[...], ww_ref[...])
    place = [place_ref[c] for c in range(3)]
    total = total_ref[...]
    way = [way_ref[c] for c in range(3)]
    pending = []
    for far in others:
        more, directions = half_edges(far, slots, rows, place, None, mats)
        total = total + more
        pending.append(directions)
    message_mean = ((total[:rows] + total[rows:]) * mean_scale).astype(BF16)
    node_pre = node_ref[...] + dot(message_mean, w_node[width:, :])
    node_hidden = half_silu(node_pre * 0.5).astype(BF16)
    change = dot(node_hidden, w_out[...])
    for directions in pending:
        way = [w + more for w, more in zip(way, directions())]
    x = jnp.concatenate([own[slots[0], k] for k in range(slabs)], axis=0)
    feat_out[...] = (x.astype(F32) + change).astype(BF16)
    lane = lax.broadcasted_iota(jnp.int32, (groups, LANES), 1)
    sums = []
    for w in way:
        parts = [
            jnp.sum(jnp.where(lane // sources == f, w, 0.0), axis=1, keepdims=True)
            for f in range(fold)
        ]
        sums.append(jnp.concatenate(parts, axis=0))
    wide = lax.broadcasted_iota(jnp.int32, (rows, LANES), 1)
    side = jnp.where(wide == 0, sums[0], jnp.where(wide == 1, sums[1], sums[2]))
    spot = own[slots[0], slabs].astype(F32)
    coord_out[...] = spot[:3, :rows] + side.T[:3] * mean_scale


def shards(
    node_feat,
    coords,
    pair_table,
    w_tgt,
    w_src,
    w_dist,
    edge_bias,
    w_edge,
    w_gate,
    w_coord,
    w_weight,
    w_node_in,
    w_node_out,
):
    rows, width = node_feat.shape
    edge_parts = lax.axis_size("edge")
    blocks = lax.axis_size("blk")
    rounds = pair_table.shape[0]
    mean_scale = 1.0 / ((rounds + 1) * rows * edge_parts - 1)
    vmem = pl.BlockSpec(memory_space=pltpu.VMEM)
    smem = pl.BlockSpec(memory_space=pltpu.SMEM)
    params = pltpu.CompilerParams(vmem_limit_bytes=VMEM_BYTES)
    line = lambda v: v.reshape(1, -1)
    small = (line(w_dist), line(edge_bias), line(w_gate), line(w_weight))
    hold = lambda v: pltpu.with_memory_space_constraint(v, pltpu.HBM)
    weights = (w_tgt, w_src, w_edge, w_coord, w_node_in, w_node_out)
    sent, lines, table, *near = pl.pallas_call(
        pack_body,
        out_shape=(
            pltpu.VMEM((blocks, rows // SLAB + 1, SLAB, width), BF16),
            pltpu.VMEM((8, width), F32),
            pltpu.SMEM(pair_table.shape, pair_table.dtype),
        )
        + tuple(pltpu.VMEM(w.shape, w.dtype) for w in weights),
        in_specs=[vmem] * 2 + [smem] + [vmem] * (4 + len(weights)),
        out_specs=(vmem, vmem, smem) + (vmem,) * len(weights),
        compiler_params=params,
        name="pack",
    )(*(hold(v) for v in (node_feat, coords, pair_table) + small + weights))
    order = [[blocks - 1] + list(range(blocks - 1))]
    far = [lax.all_to_all(sent, "blk", 0, 0, tiled=True, axis_index_groups=order)]
    for step in range(1, edge_parts):
        ring = [(e, (e + step) % edge_parts) for e in range(edge_parts)]
        far.append(lax.ppermute(far[0], "edge", ring))

    w_tgt, w_src, w_edge, w_coord, w_node, w_out = near
    fold = LANES // (rows * (rounds + 1))
    groups = rows // fold
    prepared = pl.pallas_call(
        near_body,
        out_shape=(
            pltpu.VMEM((width, 2 * rows + 16), BF16),
            pltpu.VMEM((width, width), BF16),
            pltpu.VMEM((width, width), BF16),
            pltpu.VMEM((width + 16, width), BF16),
            pltpu.VMEM((width, LANES), F32),
            pltpu.VMEM((3, groups, LANES), F32),
            pltpu.VMEM((rows, width), F32),
            pltpu.VMEM((2 * rows, width), F32),
            pltpu.VMEM((3, groups, LANES), F32),
        ),
        in_specs=[smem] + [vmem] * 7,
        out_specs=(vmem,) * 9,
        compiler_params=params,
        cost_estimate=pl.CostEstimate(
            flops=4 * rows * rows * (rounds + 1) * width * width,
            transcendentals=3 * rows * rows * (rounds + 1) * width,
            bytes_accessed=0,
        ),
        name="near",
    )(table, lines, w_tgt, w_src, w_edge, w_coord, w_node, far[0])

    def body(*refs):
        far_body(*refs, mean_scale=mean_scale)

    return pl.pallas_call(
        body,
        out_shape=(
            jax.ShapeDtypeStruct((rows, width), BF16),
            jax.ShapeDtypeStruct((3, rows), F32),
        ),
        in_specs=[smem] + [vmem] * (11 + edge_parts),
        out_specs=(vmem, vmem),
        compiler_params=params,
        name="far",
    )(table, *prepared, w_node, w_out, *far)


def solution(mesh):
    whole = P()
    placed = (P(("blk", "edge"), None), P(None, ("blk", "edge"))) + (whole,) * 11
    return jax.shard_map(
        shards,
        mesh=mesh,
        in_specs=placed,
        out_specs=(P(("blk", "edge"), None), P(None, ("blk", "edge"))),
        check_vma=False,
    )
```
